256 devices in a mesh: cells: 256 (over z, x, y, core).
Axes of the slice: x: 4, y: 4, z: 8, core: 2. Of those that a mesh axis runs over, the one named last changes fastest.
Arguments:
- field: float32 [9, 55, 262144], P(None, None, 'cells'), may hold values from -6 to 6
- cell_area: float32 [262144], P('cells'), may hold values from 0.5 to 2
- dv_edge: float32 [827392], P('cells'), may hold values from 0.6 to 1.6
- dc_edge: float32 [827392], P('cells'), may hold values from 0.6 to 1.6
- cells_on_edge: int32 [2, 827392], P(None, 'cells'), may hold values from 0 to 1407, as said below
- edges_on_cell: int32 [6, 262144], P(None, 'cells'), may hold values from 0 to 3231, as said below
- send_cells: int32 [6, 16384], P(None, 'cells'), may hold values from 0 to 1023
- level_coef: float32 [55], replicated, may hold values from 0.005 to 0.02
Outputs:
- tendency: float32 [9, 55, 262144], P(None, None, 'cells')
The draws below stay inside these ranges and needn't reach their ends.
Inputs may be any that keep to these rules, and one draw needn't show every extreme that they name: `cells_on_edge`: the blocks tile one periodic hexagonal mesh, each a parallelogram of 64 by 16 cells; block b borders b + 1 and b - 1 along the first direction, b + 16 and b - 16 along the second, and b + 15 and b - 15 at one cell each, all modulo 256. Every edge with a cell in a block is listed once in that block, with the same dv_edge and dc_edge wherever it is listed, plus one extra entry that no cell names. Cells and edges are numbered in random order in each block. `edges_on_cell`: each cell names six distinct edges of its block.
All inputs are finite; a program needn't handle non-finite values.
Results may differ from the reference program's by a relative error of at most 0.00005.
Values sent between devices are 32-bit elements; how exact they have to be, the bound alone decides.
A program may use at most 128 MiB of HBM per device.

```python
import math
import jax
import jax.numpy as jnp
import numpy as np
from jax import lax

CELLS_X = 64
CELLS_Y = 16
FIELDS = 9
LEVELS = 55
BLOCK_ROW = 16
BLOCKS = 256
CELLS_DEV = 1024
SLOT = 64
EDGES_DEV = 3232
TOTAL_CELLS = 262144


def canonical_tables():
    width = CELLS_X
    height = CELLS_Y
    cell_count = width * height
    places = np.arange(cell_count)
    column = places % width
    row_index = places // width
    step_x = np.array([1, 0, 1])
    step_y = np.array([0, 1, -1])
    owned_dir = np.tile(np.arange(3), cell_count)
    owned_sx = np.repeat(column, 3)
    owned_sy = np.repeat(row_index, 3)
    owned_tx = owned_sx + step_x[owned_dir]
    owned_ty = owned_sy + step_y[owned_dir]
    along_y = np.arange(height)
    along_x = np.arange(width)
    short_x = np.arange(width - 1)
    src_x = np.concatenate([owned_sx, -np.ones(height, np.int64), -np.ones(height, np.int64), along_x, short_x, np.zeros(1, np.int64)])
    src_y = np.concatenate([owned_sy, along_y, along_y + 1, -np.ones(width, np.int64), height * np.ones(width - 1, np.int64), np.zeros(1, np.int64)])
    dst_x = np.concatenate([owned_tx, np.zeros(height, np.int64), np.zeros(height, np.int64), along_x, short_x + 1, np.zeros(1, np.int64)])
    dst_y = np.concatenate([owned_ty, along_y, along_y, np.zeros(width, np.int64), (height - 1) * np.ones(width - 1, np.int64), np.zeros(1, np.int64)])
    edge_dir = np.concatenate([owned_dir, np.zeros(height, np.int64), 2 * np.ones(height, np.int64), np.ones(width, np.int64), 2 * np.ones(width - 1, np.int64), np.zeros(1, np.int64)])
    base = 3 * cell_count
    beside_all = np.stack([places * 3, places * 3 + 1, places * 3 + 2, np.where(column > 0, (places - 1) * 3, base + row_index), np.where(row_index > 0, (places - width) * 3 + 1, base + 2 * height + column), np.where((column > 0) & (row_index < height - 1), (places + width - 1) * 3 + 2, np.where(column == 0, base + height + row_index, base + 2 * height + width + column - 1))])
    return (src_x, src_y, dst_x, dst_y, edge_dir, beside_all)


def frame_slots(coord_x, coord_y):
    width = CELLS_X
    height = CELLS_Y
    cell_count = width * height
    slot_len = CELLS_X
    inside_y = (coord_y >= 0) & (coord_y < height)
    inside_x = (coord_x >= 0) & (coord_x < width)
    is_own = inside_x & inside_y
    own_place = np.clip(coord_y, 0, height - 1) * width + np.clip(coord_x, 0, width - 1)
    halo_index = np.where((coord_x == -1) & inside_y, cell_count + coord_y, np.where((coord_x == width) & inside_y, cell_count + slot_len + coord_y, np.where((coord_y == -1) & inside_x, cell_count + 2 * slot_len + coord_x, np.where((coord_y == height) & inside_x, cell_count + 3 * slot_len + coord_x, np.where((coord_x == width) & (coord_y == -1), cell_count + 4 * slot_len + 0 * coord_x, np.where((coord_x == -1) & (coord_y == height), cell_count + 5 * slot_len + 0 * coord_x, 0))))))
    return (is_own, own_place, halo_index)


def mesh_numbering(key):
    cell_keys = jax.random.split(jax.random.fold_in(key, 11), BLOCKS)
    edge_keys = jax.random.split(jax.random.fold_in(key, 12), BLOCKS)
    place_of_cell = jax.vmap(lambda sub: jax.random.permutation(sub, CELLS_DEV))(cell_keys).astype(jnp.int32)
    cell_of_place = jnp.argsort(place_of_cell, axis=1).astype(jnp.int32)
    canon_of_edge = jax.vmap(lambda sub: jax.random.permutation(sub, EDGES_DEV))(edge_keys).astype(jnp.int32)
    edge_of_canon = jnp.argsort(canon_of_edge, axis=1).astype(jnp.int32)
    return (place_of_cell, cell_of_place, canon_of_edge, edge_of_canon)


def draw_cells_on_edge(key, part):
    src_x, src_y, dst_x, dst_y, edge_dir, beside_all = canonical_tables()
    place_of_cell, cell_of_place, canon_of_edge, edge_of_canon = mesh_numbering(key)
    results = []
    for coord_x, coord_y in ((src_x, src_y), (dst_x, dst_y)):
        is_own, own_place, halo_index = frame_slots(coord_x, coord_y)
        own_local = jnp.take(cell_of_place, jnp.asarray(own_place, jnp.int32), axis=1)
        canon_value = jnp.where(jnp.asarray(is_own)[None, :], own_local, jnp.asarray(halo_index, jnp.int32)[None, :])
        results.append(jnp.take_along_axis(canon_value, canon_of_edge, axis=1))
    return jnp.stack(results).reshape(2, BLOCKS * EDGES_DEV).astype(jnp.int32)


def draw_edges_on_cell(key, part):
    src_x, src_y, dst_x, dst_y, edge_dir, beside_all = canonical_tables()
    place_of_cell, cell_of_place, canon_of_edge, edge_of_canon = mesh_numbering(key)
    canon_edges = jnp.take(jnp.asarray(beside_all, jnp.int32), place_of_cell, axis=1)
    local_edges = jnp.take_along_axis(jnp.broadcast_to(edge_of_canon, (6, BLOCKS, EDGES_DEV)), canon_edges, axis=2)
    return local_edges.reshape(6, BLOCKS * CELLS_DEV).astype(jnp.int32)


def draw_send_cells(key, part):
    width = CELLS_X
    height = CELLS_Y
    place_of_cell, cell_of_place, canon_of_edge, edge_of_canon = mesh_numbering(key)
    entry = np.arange(CELLS_X)
    short = np.minimum(entry, height - 1)
    positions = np.stack([short * width + width - 1, short * width, (height - 1) * width + entry, entry, (height - 1) * width + 0 * entry, width - 1 + 0 * entry])
    limits = np.array([height, height, width, width, 1, 1])
    valid = entry[None, :] < limits[:, None]
    chosen = jnp.take(cell_of_place, jnp.asarray(positions, jnp.int32), axis=1)
    chosen = jnp.where(jnp.asarray(valid)[None, :, :], chosen, 0)
    return jnp.transpose(chosen, (1, 0, 2)).reshape(6, BLOCKS * SLOT).astype(jnp.int32)


def edge_global_ids(key):
    src_x, src_y, dst_x, dst_y, edge_dir, beside_all = canonical_tables()
    place_of_cell, cell_of_place, canon_of_edge, edge_of_canon = mesh_numbering(key)
    block_x = src_x // CELLS_X
    block_y = src_y // CELLS_Y
    src_place = src_y % CELLS_Y * CELLS_X + src_x % CELLS_X
    block_step = jnp.asarray(block_x + BLOCK_ROW * block_y, jnp.int32)
    block_ids = lax.broadcasted_iota(jnp.int32, (BLOCKS, EDGES_DEV), 0)
    owner = jnp.mod(block_ids + block_step[None, :], BLOCKS)
    global_ids = (owner * CELLS_DEV + jnp.asarray(src_place, jnp.int32)[None, :]) * 3 + jnp.asarray(edge_dir, jnp.int32)[None, :]
    return jnp.take_along_axis(global_ids, canon_of_edge, axis=1).reshape(BLOCKS * EDGES_DEV)


def draw_dv_edge(key, part):
    sub = jax.random.fold_in(key, 21)
    count = BLOCKS * CELLS_DEV * 3
    table = jnp.exp(jax.random.uniform(sub, (count,), jnp.float32, math.log(0.7), math.log(1.4)))
    return jnp.take(table, edge_global_ids(key)).astype(jnp.float32)


def draw_dc_edge(key, part):
    sub = jax.random.fold_in(key, 22)
    count = BLOCKS * CELLS_DEV * 3
    table = jnp.exp(jax.random.uniform(sub, (count,), jnp.float32, math.log(0.7), math.log(1.4)))
    return jnp.take(table, edge_global_ids(key)).astype(jnp.float32)


def level_of(stream_key, shape, cuts, least, high):
    level = 1.0
    for axis_at, blocks in cuts:
        steps = jax.random.uniform(jax.random.fold_in(jax.random.fold_in(stream_key, 6), axis_at), (blocks,), jnp.float32, least / len(cuts), high / len(cuts))
        level = level * jnp.repeat(jnp.exp(steps), shape[axis_at] // blocks).reshape((-1,) + (1,) * (len(shape) - 1 - axis_at))
    return level


def bell_draw(key, shape, scale, most, cuts=(), held_as=jnp.bfloat16):
    values = scale * jax.random.normal(key, shape, jnp.float32)
    if cuts:
        values = values * level_of(key, shape, cuts, -0.22, 0.18)
    return jnp.clip(values, -most, most).astype(held_as)


def setup_inputs(seed: int = 0) -> dict:
    arg_keys = jax.random.split(jax.random.key(seed), 9)
    field = bell_draw(arg_keys[0], (FIELDS, LEVELS, TOTAL_CELLS), 1.0, 6.0, ((2, 256),), jnp.float32)
    cell_area = jnp.clip(jnp.exp(math.log(2.0) - 1.3862944 * jax.random.uniform(arg_keys[1], (TOTAL_CELLS,), jnp.float32) ** level_of(arg_keys[1], (TOTAL_CELLS,), ((0, 256),), -0.2, 0.2)), 0.5, 2.0)
    dv_edge = draw_dv_edge(jax.random.fold_in(arg_keys[8], 71), 0)
    dc_edge = draw_dc_edge(jax.random.fold_in(arg_keys[8], 71), 0)
    cells_on_edge = draw_cells_on_edge(jax.random.fold_in(arg_keys[8], 71), 0)
    edges_on_cell = draw_edges_on_cell(jax.random.fold_in(arg_keys[8], 71), 0)
    send_cells = draw_send_cells(jax.random.fold_in(arg_keys[8], 71), 0)
    level_coef = jnp.clip(jnp.exp(jax.random.uniform(arg_keys[7], (LEVELS,), jnp.float32, math.log(0.005), math.log(0.02))), 0.005, 0.02)
    return {"field": field, "cell_area": cell_area, "dv_edge": dv_edge, "dc_edge": dc_edge, "cells_on_edge": cells_on_edge, "edges_on_cell": edges_on_cell, "send_cells": send_cells, "level_coef": level_coef}


def reference(field, cell_area, dv_edge, dc_edge, cells_on_edge, edges_on_cell, send_cells, level_coef):
    blocks = BLOCKS
    weight = (dv_edge / dc_edge).reshape(blocks, EDGES_DEV)
    area_block = cell_area.reshape(blocks, CELLS_DEV)
    endpoints = cells_on_edge.reshape(2, blocks, EDGES_DEV)
    beside_all = edges_on_cell.reshape(6, blocks, CELLS_DEV)
    send_lists = send_cells.reshape(6, blocks, SLOT)
    offsets = (1, -1, BLOCK_ROW, -BLOCK_ROW, BLOCK_ROW - 1, 1 - BLOCK_ROW)
    first_end = jnp.take_along_axis(jnp.broadcast_to(endpoints[0], (6, blocks, EDGES_DEV)), beside_all, axis=2)
    own_index = lax.broadcasted_iota(jnp.int32, (6, blocks, CELLS_DEV), 2)
    orient = jnp.where(first_end == own_index, 1.0, -1.0).astype(jnp.float32)

    def laplacian(values):
        pieces = [values]
        for direction in range(6):
            source = jnp.roll(values, offsets[direction], axis=0)
            chosen = jnp.roll(send_lists[direction], offsets[direction], axis=0)
            pieces.append(jnp.take_along_axis(source, chosen, axis=1))
        extended = jnp.concatenate(pieces, axis=1)
        upper_end = jnp.take_along_axis(extended, endpoints[1], axis=1)
        lower_end = jnp.take_along_axis(extended, endpoints[0], axis=1)
        fluxes = weight * (upper_end - lower_end)
        gathered = jnp.take_along_axis(jnp.broadcast_to(fluxes, (6, blocks, EDGES_DEV)), beside_all, axis=2)
        return jnp.sum(orient * gathered, axis=0) / area_block

    def one_level(packed):
        values, factor = packed
        return -factor * laplacian(laplacian(values))

    level_rows = field.reshape(FIELDS * LEVELS, blocks, CELLS_DEV)
    factors = jnp.tile(level_coef, FIELDS)
    result = lax.map(one_level, (level_rows, factors))
    return result.reshape(FIELDS, LEVELS, blocks * CELLS_DEV)
```

```python
import functools

import jax
import jax.numpy as jnp
from jax import lax
from jax.experimental import pallas as pl
from jax.experimental.pallas import tpu as pltpu
from jax.sharding import PartitionSpec as P

MESH = pl.DeviceIdType.MESH
F32 = jnp.float32
BF16 = jnp.bfloat16
I32 = jnp.int32

BLOCK_ROW = 16
SIDE = 16
SLOT = 64
CELLS = 1024
HALO = 256
DEPTH = CELLS + HALO
FIELDS = 9
LEVELS = 55
PITCH = 56
ROWS = 512
EDGES = 3232
GROUPS = -(-EDGES // 128)
CORNER_A = CELLS + 192
CORNER_B = CELLS + 224


def dot(a, b):
    return jnp.dot(a, b, preferred_element_type=F32)


def split(x):
    high = x.astype(BF16)
    return high, (x - high.astype(F32)).astype(BF16)


def lanes(shape):
    return lax.broadcasted_iota(I32, shape, 1)


def rows_of(shape):
    return lax.broadcasted_iota(I32, shape, 0)


def kernel(
    field,
    area,
    dv,
    dc,
    ends,
    beside,
    send,
    out,
    xf,
    xh,
    xl,
    select,
    lh,
    ll,
    near,
    coef,
    diag,
    acc,
    halo_h,
    halo_l,
    send_up,
    send_down,
    send_right,
    send_left,
    send_corner,
    got_up,
    got_down,
    got_right,
    got_left,
    got_corner,
    load_sem,
    send_sem,
    recv_sem,
):
    count = lax.axis_size("cells")
    me = lax.axis_index("cells")

    def at(offset):
        return lax.rem(me + (offset + count), count)

    offsets = (1, -1, BLOCK_ROW, -BLOCK_ROW, BLOCK_ROW - 1, 1 - BLOCK_ROW)
    barrier = pltpu.get_barrier_semaphore()
    for offset in offsets:
        pl.semaphore_signal(barrier, inc=1, device_id=(at(offset),), device_id_type=MESH)

    loads = []
    for f in range(FIELDS):
        loads.append(pltpu.make_async_copy(field.at[f], xf.at[f], load_sem.at[f]))
        loads[-1].start()

    lists = send[...]
    wide = (1, 128)
    lane1 = lanes(wide)
    first_cols = jnp.concatenate([lists[2:3], lists[3:4]], axis=1)
    second_cols = jnp.concatenate([lists[0:1], lists[1:2]], axis=1)
    near_cols = jnp.where(lane1 < 16, second_cols, pltpu.roll(second_cols, 80, 1))
    corner_cols = jnp.where(
        lane1 < 96,
        jnp.broadcast_to(lists[4:5, 0:1], wide),
        jnp.broadcast_to(lists[5:6, 0:1], wide),
    )
    second_cols = jnp.where(lane1 < 32, near_cols, jnp.where(lane1 < 64, -1, corner_cols))
    columns = jnp.concatenate([first_cols, second_cols], axis=1)

    def fill_select(i, carry):
        at_row = pl.multiple_of(i * 16, 16)
        ids = rows_of((16, HALO)) + at_row
        select[pl.ds(at_row, 16), :] = jnp.where(ids == columns, 1.0, 0.0).astype(BF16)
        return carry

    lax.fori_loop(0, CELLS // 16, fill_select, 0, unroll=4)

    pad = jnp.zeros((1, CELLS), F32)
    for f in range(FIELDS):
        loads[f].wait()
        acc[pl.ds(f * PITCH, PITCH), :] = jnp.concatenate([xf[f], pad], axis=0)
    acc[pl.ds(FIELDS * PITCH, ROWS - FIELDS * PITCH), :] = jnp.zeros(
        (ROWS - FIELDS * PITCH, CELLS), F32
    )
    high, low = split(acc[...])
    xh[...] = high
    xl[...] = low

    lane = lanes((256, 128))

    def exchange(k):
        picked = dot(xh[...], select[...]) + dot(xl[...], select[...])
        top = picked[:256, :128]
        low_half = picked[256:, :128]
        send_up[k] = jnp.where(lane < 64, top, pltpu.roll(low_half, 64, 1))
        send_down[k] = jnp.where(lane < 64, pltpu.roll(top, 64, 1), low_half)
        rest = picked[:, 128:]
        group = lanes((64, 128)) // 16
        right = rest[0:64]
        left = pltpu.roll(rest[0:64], 112, 1)
        for g in range(1, 8):
            part = rest[64 * g : 64 * g + 64]
            right = jnp.where(group == g, pltpu.roll(part, 16 * g, 1), right)
            left = jnp.where(group == g, part if g == 1 else pltpu.roll(part, 16 * g - 16, 1), left)
        send_right[k] = right
        send_left[k] = left
        lane32 = lanes((32, 128))
        own = (lane32 >= 64) & ((lane32 & 31) == rows_of((32, 128)))
        folded = [
            jnp.sum(jnp.where(own, rest[32 * g : 32 * g + 32], 0.0), axis=0, keepdims=True)
            for g in range(16)
        ]
        send_corner[k] = jnp.concatenate(folded, axis=0)
        if k == 0:
            pl.semaphore_wait(barrier, 6)
        plan = (
            (send_up, got_up, None, offsets[2]),
            (send_down, got_down, None, offsets[3]),
            (send_right, got_right, None, offsets[0]),
            (send_left, got_left, None, offsets[1]),
            (send_corner, got_corner, 0, offsets[4]),
            (send_corner, got_corner, 1, offsets[5]),
        )
        copies = []
        for i, (src, dst, which, offset) in enumerate(plan):
            copies.append(
                pltpu.make_async_remote_copy(
                    src_ref=src.at[k],
                    dst_ref=dst.at[k] if which is None else dst.at[k, which],
                    send_sem=send_sem.at[k, i],
                    recv_sem=recv_sem.at[k, i],
                    device_id=(at(offset),),
                    device_id_type=MESH,
                )
            )
            copies[-1].start()
        return copies

    def receive(k, copies):
        for copy in copies:
            copy.wait_recv()
        up = got_up[k]
        down = got_down[k]
        halo_top = jnp.where(lane < 64, up, pltpu.roll(down, 64, 1))
        halo_low = jnp.where(lane < 64, pltpu.roll(up, 64, 1), down)
        for part, start in ((halo_top, 0), (halo_low, 256)):
            high, low = split(part)
            halo_h[pl.ds(start, 256), 0:128] = high
            halo_l[pl.ds(start, 256), 0:128] = low
        right = got_right[k]
        left = got_left[k]
        corner_a = got_corner[k, 0]
        corner_b = got_corner[k, 1]
        lane64 = lanes((64, 128))
        own = (lane64 & 31) == (rows_of((64, 128)) & 31)
        upper = rows_of((64, 128)) < 32
        lane2 = lanes((2, 128))
        for g in range(8):
            corners = jnp.where(lane2 < 96, corner_a[2 * g : 2 * g + 2], corner_b[2 * g : 2 * g + 2])
            spread = jnp.where(
                upper,
                jnp.broadcast_to(corners[0:1], (64, 128)),
                jnp.broadcast_to(corners[1:2], (64, 128)),
            )
            spread = jnp.where(own, spread, 0.0)
            from_left = right if g == 0 else pltpu.roll(right, 128 - 16 * g, 1)
            from_right = left if g == 1 else pltpu.roll(left, (144 - 16 * g) % 128, 1)
            part = jnp.where(
                lane64 < 16,
                from_left,
                jnp.where(lane64 < 32, from_right, jnp.where(lane64 < 64, 0.0, spread)),
            )
            high, low = split(part)
            halo_h[pl.ds(64 * g, 64), 128:256] = high
            halo_l[pl.ds(64 * g, 64), 128:256] = low

    copies_a = exchange(0)

    packed = []
    weights = []
    for r in range(GROUPS):
        width = min(128, EDGES - 128 * r)
        where = slice(128 * r, 128 * r + width)
        both = ends[0:1, where] | (ends[1:2, where] << 11)
        ratio = dv[0:1, where] / dc[0:1, where]
        if width < 128:
            both = jnp.concatenate([both, jnp.zeros((1, 128 - width), I32)], axis=1)
            ratio = jnp.concatenate([ratio, jnp.zeros((1, 128 - width), F32)], axis=1)
        packed.append(jnp.broadcast_to(both, (8, 128)))
        weights.append(jnp.broadcast_to(ratio, (8, 128)))
    edge_ids = jnp.concatenate([beside[...], jnp.zeros((2, CELLS), I32)], axis=0)
    tile = (8, 128)
    valid = rows_of(tile) < 6
    for t in range(CELLS // 128):
        cols = slice(128 * t, 128 * t + 128)
        ids = edge_ids[:, cols]
        group = ids >> 7
        within = ids & 127
        both = jnp.zeros(tile, I32)
        ratio = jnp.zeros(tile, F32)
        for r in range(GROUPS):
            here = group == r
            both = jnp.where(here, jnp.take_along_axis(packed[r], within, axis=1), both)
            ratio = jnp.where(here, jnp.take_along_axis(weights[r], within, axis=1), ratio)
        end0 = both & 2047
        end1 = both >> 11
        other = jnp.where(end0 == lanes(tile) + 128 * t, end1, end0)
        beyond = other - CELLS
        slot = beyond >> 6
        place = beyond & 63
        start = jnp.where(
            slot == 2,
            CELLS,
            jnp.where(
                slot == 3,
                CELLS + 64,
                jnp.where(
                    slot == 0,
                    CELLS + 128,
                    jnp.where(slot == 1, CELLS + 144, jnp.where(slot == 4, CORNER_A, CORNER_B)),
                ),
            ),
        )
        other = jnp.where(other < CELLS, other, start + place)
        near[:, cols] = jnp.where(valid, other, -1)
        factor = jnp.where(valid, ratio / area[0:1, cols], 0.0)
        high, low = split(factor)
        factor = high.astype(F32) + low.astype(F32)
        coef[:, cols] = factor
        diag[0:1, cols] = jnp.sum(factor, axis=0, keepdims=True)

    for t in range(CELLS // 128):
        cols = slice(128 * t, 128 * t + 128)
        nears = [jnp.broadcast_to(near[j : j + 1, cols], (16, 128)) for j in range(6)]
        coefs = [jnp.broadcast_to(coef[j : j + 1, cols], (16, 128)) for j in range(6)]

        def put(at_row, ids, cols=cols, nears=nears, coefs=coefs):
            value = jnp.where(ids == nears[0], coefs[0], 0.0)
            for j in range(1, 6):
                value = jnp.where(ids == nears[j], coefs[j], value)
            high, low = split(value)
            lh[pl.ds(at_row, 16), cols] = high
            ll[pl.ds(at_row, 16), cols] = low

        def fill(i, carry, put=put):
            at_row = pl.multiple_of(i * 16, 16)
            put(at_row, rows_of((16, 128)) + at_row)
            return carry

        lax.fori_loop(0, CORNER_A // 16, fill, 0, unroll=4)
        for at_row in range(CORNER_A, DEPTH, 16):
            put(at_row, jnp.full((16, 128), CORNER_A if at_row < CORNER_B else CORNER_B, I32))

    tiles = [slice(256 * n, 256 * n + 256) for n in range(CELLS // 256)]

    def own_part():
        for cols in tiles:
            a = dot(xh[...], lh[0:CELLS, cols])
            a += dot(xh[...], ll[0:CELLS, cols])
            a += dot(xl[...], lh[0:CELLS, cols])
            acc[:, cols] = a - diag[0:1, cols] * acc[:, cols]

    def halo_part(cols):
        a = dot(halo_h[...], lh[CELLS:DEPTH, cols])
        a += dot(halo_h[...], ll[CELLS:DEPTH, cols])
        a += dot(halo_l[...], lh[CELLS:DEPTH, cols])
        return acc[:, cols] + a

    own_part()
    receive(0, copies_a)
    for cols in tiles:
        value = halo_part(cols)
        acc[:, cols] = value
        high, low = split(value)
        xh[:, cols] = high
        xl[:, cols] = low
    copies_b = exchange(1)
    own_part()
    receive(1, copies_b)
    for cols in tiles:
        value = halo_part(cols)
        for f in range(FIELDS):
            out[f, :, cols] = value[f * PITCH : f * PITCH + LEVELS]
    for copy in copies_a + copies_b:
        copy.wait_send()


def shards(
    field, cell_area, dv_edge, dc_edge, cells_on_edge, edges_on_cell, send_cells, level_coef
):
    vmem = pl.BlockSpec(memory_space=pltpu.VMEM)
    second = pl.pallas_call(
        kernel,
        out_shape=jax.ShapeDtypeStruct(field.shape, F32),
        in_specs=[pl.BlockSpec(memory_space=pl.ANY)] + [vmem] * 6,
        out_specs=vmem,
        scratch_shapes=[
            pltpu.VMEM((FIELDS, LEVELS, CELLS), F32),
            pltpu.VMEM((ROWS, CELLS), BF16),
            pltpu.VMEM((ROWS, CELLS), BF16),
            pltpu.VMEM((CELLS, HALO), BF16),
            pltpu.VMEM((DEPTH, CELLS), BF16),
            pltpu.VMEM((DEPTH, CELLS), BF16),
            pltpu.VMEM((8, CELLS), I32),
            pltpu.VMEM((8, CELLS), F32),
            pltpu.VMEM((1, CELLS), F32),
            pltpu.VMEM((ROWS, CELLS), F32),
            pltpu.VMEM((ROWS, HALO), BF16),
            pltpu.VMEM((ROWS, HALO), BF16),
            pltpu.VMEM((2, 256, 128), F32),
            pltpu.VMEM((2, 256, 128), F32),
            pltpu.VMEM((2, 64, 128), F32),
            pltpu.VMEM((2, 64, 128), F32),
            pltpu.VMEM((2, 16, 128), F32),
            pltpu.VMEM((2, 256, 128), F32),
            pltpu.VMEM((2, 256, 128), F32),
            pltpu.VMEM((2, 64, 128), F32),
            pltpu.VMEM((2, 64, 128), F32),
            pltpu.VMEM((2, 2, 16, 128), F32),
            pltpu.SemaphoreType.DMA((FIELDS,)),
            pltpu.SemaphoreType.DMA((2, 6)),
            pltpu.SemaphoreType.DMA((2, 6)),
        ],
        compiler_params=pltpu.CompilerParams(
            collective_id=0, has_side_effects=True, vmem_limit_bytes=48 * 1024 * 1024
        ),
        name="diffusion",
    )(
        field,
        cell_area.reshape(1, -1),
        dv_edge.reshape(1, -1),
        dc_edge.reshape(1, -1),
        cells_on_edge,
        edges_on_cell,
        send_cells,
    )
    return -level_coef[None, :, None] * second


def solution(mesh):
    return jax.shard_map(
        shards,
        mesh=mesh,
        in_specs=(
            P(None, None, "cells"),
            P("cells"),
            P("cells"),
            P("cells"),
            P(None, "cells"),
            P(None, "cells"),
            P(None, "cells"),
            P(),
        ),
        out_specs=P(None, None, "cells"),
        check_vma=False,
    )
```

```python
import functools

import jax
import jax.numpy as jnp
from jax import lax
from jax.experimental import pallas as pl
from jax.experimental.pallas import tpu as pltpu
from jax.sharding import PartitionSpec as P

MESH = pl.DeviceIdType.MESH
F32 = jnp.float32
BF16 = jnp.bfloat16
I32 = jnp.int32

BLOCK_ROW = 16
SIDE = 16
SLOT = 64
CELLS = 1024
HALO = 256
FIELDS = 9
LEVELS = 55
PITCH = 56
ROWS = 512
CHUNKS = 2
CHUNK = ROWS // CHUNKS
EDGES = 3232
GROUPS = -(-EDGES // 128)
CORNER_A = CELLS + 192
CORNER_B = CELLS + 224


def dot(a, b):
    return jnp.dot(a, b, preferred_element_type=F32)


def split(x):
    high = x.astype(BF16)
    return high, (x - high.astype(F32)).astype(BF16)


def lanes(shape):
    return lax.broadcasted_iota(I32, shape, 1)


def rows_of(shape):
    return lax.broadcasted_iota(I32, shape, 0)


def kernel(
    field,
    area_in,
    dv_in,
    dc_in,
    ends_in,
    beside_in,
    send_in,
    acc,
    halo_h,
    halo_l,
    rim_h,
    rim_l,
    area,
    dv,
    dc,
    ends,
    beside,
    send,
    xf,
    xh,
    xl,
    select,
    lh,
    ll,
    near,
    coef,
    diag,
    send_up,
    send_down,
    send_right,
    send_left,
    send_corner,
    got_up,
    got_down,
    got_right,
    got_left,
    got_corner,
    load_sem,
    send_sem,
    recv_sem,
):
    count = lax.axis_size("cells")
    me = lax.axis_index("cells")

    def at(offset):
        return lax.rem(me + (offset + count), count)

    offsets = (1, -1, BLOCK_ROW, -BLOCK_ROW, BLOCK_ROW - 1, 1 - BLOCK_ROW)
    barrier = pltpu.get_barrier_semaphore()
    for offset in offsets:
        pl.semaphore_signal(barrier, inc=1, device_id=(at(offset),), device_id_type=MESH)

    def load(i, src, dst):
        copy = pltpu.make_async_copy(src, dst, load_sem.at[i])
        copy.start()
        return copy

    list_load = load(FIELDS, send_in, send)
    loads = [load(f, field.at[f], xf.at[f]) for f in range(FIELDS)]
    table_loads = [
        load(FIELDS + 1 + i, src, dst)
        for i, (src, dst) in enumerate(
            ((beside_in, beside), (ends_in, ends), (dv_in, dv), (dc_in, dc), (area_in, area))
        )
    ]

    list_load.wait()
    lists = send[...]
    wide = (1, 128)
    lane1 = lanes(wide)
    first_cols = jnp.concatenate([lists[2:3], lists[3:4]], axis=1)
    second_cols = jnp.concatenate([lists[0:1], lists[1:2]], axis=1)
    near_cols = jnp.where(lane1 < 16, second_cols, pltpu.roll(second_cols, 80, 1))
    corner_cols = jnp.where(
        lane1 < 96,
        jnp.broadcast_to(lists[4:5, 0:1], wide),
        jnp.broadcast_to(lists[5:6, 0:1], wide),
    )
    second_cols = jnp.where(lane1 < 32, near_cols, jnp.where(lane1 < 64, -1, corner_cols))
    columns = jnp.concatenate([first_cols, second_cols], axis=1)

    def fill_select(i, carry):
        at_row = pl.multiple_of(i * 16, 16)
        ids = rows_of((16, HALO)) + at_row
        select[pl.ds(at_row, 16), :] = jnp.where(ids == columns, 1.0, 0.0).astype(BF16)
        return carry

    lax.fori_loop(0, CELLS // 16, fill_select, 0, unroll=8)

    half = CHUNK // 2
    part = CHUNK // 8
    corner_rows = CHUNK // 32

    def exchange(k, h):
        here = pl.ds(h * CHUNK, CHUNK)
        picked = dot(xh[here, :], select[...]) + dot(xl[here, :], select[...])
        lane = lanes((half, 128))
        top = picked[:half, :128]
        low_half = picked[half:, :128]
        send_up[k, h] = jnp.where(lane < 64, top, pltpu.roll(low_half, 64, 1))
        send_down[k, h] = jnp.where(lane < 64, pltpu.roll(top, 64, 1), low_half)
        rest = picked[:, 128:]
        group = lanes((part, 128)) // 16
        right = rest[0:part]
        left = pltpu.roll(rest[0:part], 112, 1)
        for g in range(1, 8):
            piece = rest[part * g : part * g + part]
            right = jnp.where(group == g, pltpu.roll(piece, 16 * g, 1), right)
            left = jnp.where(group == g, piece if g == 1 else pltpu.roll(piece, 16 * g - 16, 1), left)
        send_right[k, h] = right
        send_left[k, h] = left
        lane32 = lanes((32, 128))
        own = (lane32 >= 64) & ((lane32 & 31) == rows_of((32, 128)))
        folded = [
            jnp.sum(jnp.where(own, rest[32 * g : 32 * g + 32], 0.0), axis=0, keepdims=True)
            for g in range(corner_rows)
        ]
        send_corner[k, h] = jnp.concatenate(folded, axis=0)
        if k == 0 and h == 0:
            pl.semaphore_wait(barrier, 6)
        plan = (
            (send_up, got_up.at[k, h], offsets[2]),
            (send_down, got_down.at[k, h], offsets[3]),
            (send_right, got_right.at[k, h], offsets[0]),
            (send_left, got_left.at[k, h], offsets[1]),
            (send_corner, got_corner.at[k, h, 0], offsets[4]),
            (send_corner, got_corner.at[k, h, 1], offsets[5]),
        )
        copies = []
        for i, (src, dst, offset) in enumerate(plan):
            copies.append(
                pltpu.make_async_remote_copy(
                    src_ref=src.at[k, h],
                    dst_ref=dst,
                    send_sem=send_sem.at[k, h, i],
                    recv_sem=recv_sem.at[k, h, i],
                    device_id=(at(offset),),
                    device_id_type=MESH,
                )
            )
            copies[-1].start()
        return copies

    def receive(k, h, copies):
        for copy in copies:
            copy.wait_recv()
        lane = lanes((half, 128))
        up = got_up[k, h]
        down = got_down[k, h]
        halo_top = jnp.where(lane < 64, up, pltpu.roll(down, 64, 1))
        halo_low = jnp.where(lane < 64, pltpu.roll(up, 64, 1), down)
        for piece, start in ((halo_top, 0), (halo_low, half)):
            high, low = split(piece)
            halo_h[pl.ds(h * CHUNK + start, half), 0:128] = high
            halo_l[pl.ds(h * CHUNK + start, half), 0:128] = low
        right = got_right[k, h]
        left = got_left[k, h]
        corner_a = got_corner[k, h, 0]
        corner_b = got_corner[k, h, 1]
        shape = (part, 128)
        lane = lanes(shape)
        own = (lane & 31) == rows_of(shape)
        corners = jnp.where(lanes((corner_rows, 128)) < 96, corner_a, corner_b)
        for g in range(8):
            spread = jnp.where(own, jnp.broadcast_to(corners[g : g + 1], shape), 0.0)
            from_left = right if g == 0 else pltpu.roll(right, 128 - 16 * g, 1)
            from_right = left if g == 1 else pltpu.roll(left, (144 - 16 * g) % 128, 1)
            piece = jnp.where(
                lane < 16,
                from_left,
                jnp.where(lane < 32, from_right, jnp.where(lane < 64, 0.0, spread)),
            )
            high, low = split(piece)
            halo_h[pl.ds(h * CHUNK + part * g, part), 128:256] = high
            halo_l[pl.ds(h * CHUNK + part * g, part), 128:256] = low

    pad = jnp.zeros((PITCH - LEVELS, CELLS), F32)
    acc[FIELDS * PITCH : ROWS, :] = jnp.zeros((ROWS - FIELDS * PITCH, CELLS), F32)
    copies_a = []
    waited = 0
    for h in range(CHUNKS):
        while waited < FIELDS and waited * PITCH < (h + 1) * CHUNK:
            loads[waited].wait()
            acc[pl.ds(waited * PITCH, PITCH), :] = jnp.concatenate([xf[waited], pad], axis=0)
            waited += 1
        here = pl.ds(h * CHUNK, CHUNK)
        high, low = split(acc[here, :])
        xh[here, :] = high
        xl[here, :] = low
        copies_a.append(exchange(0, h))

    for copy in table_loads:
        copy.wait()
    packed = []
    weights = []
    for r in range(GROUPS):
        width = min(128, EDGES - 128 * r)
        where = slice(128 * r, 128 * r + width)
        both = ends[0:1, where] | (ends[1:2, where] << 11)
        ratio = (dv[where] / dc[where]).reshape(1, width)
        if width < 128:
            both = jnp.concatenate([both, jnp.zeros((1, 128 - width), I32)], axis=1)
            ratio = jnp.concatenate([ratio, jnp.zeros((1, 128 - width), F32)], axis=1)
        packed.append(jnp.broadcast_to(both, (8, 128)))
        weights.append(jnp.broadcast_to(ratio, (8, 128)))
    edge_ids = jnp.concatenate([beside[...], jnp.zeros((2, CELLS), I32)], axis=0)
    tile = (8, 128)
    valid = rows_of(tile) < 6
    for t in range(CELLS // 128):
        cols = slice(128 * t, 128 * t + 128)
        ids = edge_ids[:, cols]
        group = ids >> 7
        within = ids & 127
        both = jnp.zeros(tile, I32)
        ratio = jnp.zeros(tile, F32)
        for r in range(GROUPS):
            here = group == r
            both = jnp.where(here, jnp.take_along_axis(packed[r], within, axis=1), both)
            ratio = jnp.where(here, jnp.take_along_axis(weights[r], within, axis=1), ratio)
        end0 = both & 2047
        end1 = both >> 11
        other = jnp.where(end0 == lanes(tile) + 128 * t, end1, end0)
        beyond = other - CELLS
        slot = beyond >> 6
        place = beyond & 63
        start = jnp.where(
            slot == 2,
            CELLS,
            jnp.where(
                slot == 3,
                CELLS + 64,
                jnp.where(
                    slot == 0,
                    CELLS + 128,
                    jnp.where(slot == 1, CELLS + 144, jnp.where(slot == 4, CORNER_A, CORNER_B)),
                ),
            ),
        )
        other = jnp.where(other < CELLS, other, start + place)
        near[:, cols] = jnp.where(valid, other, -1)
        factor = jnp.where(valid, ratio / area[cols].reshape(1, 128), 0.0)
        high, low = split(factor)
        factor = high.astype(F32) + low.astype(F32)
        coef[:, cols] = factor
        diag[0:1, cols] = jnp.sum(factor, axis=0, keepdims=True)

    for t in range(CELLS // 128):
        cols = slice(128 * t, 128 * t + 128)
        nears = [jnp.broadcast_to(near[j : j + 1, cols], (16, 128)) for j in range(6)]
        coefs = [jnp.broadcast_to(coef[j : j + 1, cols], (16, 128)) for j in range(6)]

        def put(high_ref, low_ref, at_row, ids, cols=cols, nears=nears, coefs=coefs):
            value = jnp.where(ids == nears[0], coefs[0], 0.0)
            for j in range(1, 6):
                value = jnp.where(ids == nears[j], coefs[j], value)
            high, low = split(value)
            high_ref[pl.ds(at_row, 16), cols] = high
            low_ref[pl.ds(at_row, 16), cols] = low

        def fill(i, carry, put=put):
            at_row = pl.multiple_of(i * 16, 16)
            put(lh, ll, at_row, rows_of((16, 128)) + at_row)
            return carry

        lax.fori_loop(0, CELLS // 16, fill, 0, unroll=8)
        for at_row in range(0, HALO, 16):
            ids = rows_of((16, 128)) + (CELLS + at_row)
            if CELLS + at_row >= CORNER_A:
                corner = CORNER_A if CELLS + at_row < CORNER_B else CORNER_B
                ids = jnp.full((16, 128), corner, I32)
            put(rim_h, rim_l, at_row, ids)

    tiles = [slice(256 * n, 256 * n + 256) for n in range(CELLS // 256)]

    def own_part():
        for cols in tiles:
            a = dot(xh[...], lh[:, cols])
            a += dot(xh[...], ll[:, cols])
            a += dot(xl[...], lh[:, cols])
            acc[:, cols] = a - diag[0:1, cols] * acc[:, cols]

    own_part()
    copies_b = []
    for h in range(CHUNKS):
        receive(0, h, copies_a[h])
        here = pl.ds(h * CHUNK, CHUNK)
        for cols in tiles:
            a = dot(halo_h[here, :], rim_h[:, cols])
            a += dot(halo_h[here, :], rim_l[:, cols])
            a += dot(halo_l[here, :], rim_h[:, cols])
            value = acc[here, cols] + a
            acc[here, cols] = value
            high, low = split(value)
            xh[here, cols] = high
            xl[here, cols] = low
        copies_b.append(exchange(1, h))
    own_part()
    for h in range(CHUNKS):
        receive(1, h, copies_b[h])
    for h in range(CHUNKS):
        for copy in copies_a[h] + copies_b[h]:
            copy.wait_send()


def finish(acc, halo_h, halo_l, rim_h, rim_l, level, out, result, sem):
    spread = jnp.broadcast_to(level[...], (LEVELS, LEVELS))
    on_diagonal = lanes((LEVELS, LEVELS)) == rows_of((LEVELS, LEVELS))
    scale = -jnp.sum(jnp.where(on_diagonal, spread, 0.0), axis=1, keepdims=True)
    copies = []
    for n in range(CELLS // 256):
        cols = slice(256 * n, 256 * n + 256)
        a = dot(halo_h[...], rim_h[:, cols])
        a += dot(halo_h[...], rim_l[:, cols])
        a += dot(halo_l[...], rim_h[:, cols])
        value = acc[:, cols] + a
        for f in range(FIELDS):
            result[f, :, cols] = value[f * PITCH : f * PITCH + LEVELS] * scale
        copies.append(
            pltpu.make_async_copy(result.at[:, :, cols], out.at[:, :, cols], sem.at[n])
        )
        copies[-1].start()
    for copy in copies:
        copy.wait()


def shards(
    field, cell_area, dv_edge, dc_edge, cells_on_edge, edges_on_cell, send_cells, level_coef
):
    vmem = pl.BlockSpec(memory_space=pltpu.VMEM)
    hbm = pl.BlockSpec(memory_space=pltpu.HBM)
    half = CHUNK // 2
    part = CHUNK // 8
    corner_rows = CHUNK // 32
    ends = (2, CHUNKS)
    parts = pl.pallas_call(
        kernel,
        out_shape=[
            jax.ShapeDtypeStruct((ROWS, CELLS), F32),
            jax.ShapeDtypeStruct((ROWS, HALO), BF16),
            jax.ShapeDtypeStruct((ROWS, HALO), BF16),
            jax.ShapeDtypeStruct((HALO, CELLS), BF16),
            jax.ShapeDtypeStruct((HALO, CELLS), BF16),
        ],
        in_specs=[hbm] * 7,
        out_specs=[vmem] * 5,
        scratch_shapes=[
            pltpu.VMEM((CELLS,), F32),
            pltpu.VMEM((EDGES,), F32),
            pltpu.VMEM((EDGES,), F32),
            pltpu.VMEM((2, EDGES), I32),
            pltpu.VMEM((6, CELLS), I32),
            pltpu.VMEM((6, SLOT), I32),
            pltpu.VMEM((FIELDS, LEVELS, CELLS), F32),
            pltpu.VMEM((ROWS, CELLS), BF16),
            pltpu.VMEM((ROWS, CELLS), BF16),
            pltpu.VMEM((CELLS, HALO), BF16),
            pltpu.VMEM((CELLS, CELLS), BF16),
            pltpu.VMEM((CELLS, CELLS), BF16),
            pltpu.VMEM((8, CELLS), I32),
            pltpu.VMEM((8, CELLS), F32),
            pltpu.VMEM((1, CELLS), F32),
            pltpu.VMEM((*ends, half, 128), F32),
            pltpu.VMEM((*ends, half, 128), F32),
            pltpu.VMEM((*ends, part, 128), F32),
            pltpu.VMEM((*ends, part, 128), F32),
            pltpu.VMEM((*ends, corner_rows, 128), F32),
            pltpu.VMEM((*ends, half, 128), F32),
            pltpu.VMEM((*ends, half, 128), F32),
            pltpu.VMEM((*ends, part, 128), F32),
            pltpu.VMEM((*ends, part, 128), F32),
            pltpu.VMEM((*ends, 2, corner_rows, 128), F32),
            pltpu.SemaphoreType.DMA((FIELDS + 6,)),
            pltpu.SemaphoreType.DMA((*ends, 6)),
            pltpu.SemaphoreType.DMA((*ends, 6)),
        ],
        compiler_params=pltpu.CompilerParams(
            collective_id=0, has_side_effects=True, vmem_limit_bytes=40 * 1024 * 1024
        ),
        name="diffusion",
    )(
        *(
            pltpu.with_memory_space_constraint(x, pltpu.HBM)
            for x in (
                field, cell_area, dv_edge, dc_edge, cells_on_edge, edges_on_cell, send_cells
            )
        )
    )
    return pl.pallas_call(
        finish,
        out_shape=jax.ShapeDtypeStruct(field.shape, F32),
        in_specs=[vmem] * 6,
        out_specs=hbm,
        scratch_shapes=[
            pltpu.VMEM((FIELDS, LEVELS, CELLS), F32),
            pltpu.SemaphoreType.DMA((CELLS // 256,)),
        ],
        compiler_params=pltpu.CompilerParams(vmem_limit_bytes=40 * 1024 * 1024),
        name="finish",
    )(*parts, level_coef.reshape(1, -1))


def solution(mesh):
    return jax.shard_map(
        shards,
        mesh=mesh,
        in_specs=(
            P(None, None, "cells"),
            P("cells"),
            P("cells"),
            P("cells"),
            P(None, "cells"),
            P(None, "cells"),
            P(None, "cells"),
            P(),
        ),
        out_specs=P(None, None, "cells"),
        check_vma=False,
    )
```

```python
import functools

import jax
import jax.numpy as jnp
from jax import lax
from jax.experimental import pallas as pl
from jax.experimental.pallas import tpu as pltpu
from jax.sharding import PartitionSpec as P

MESH = pl.DeviceIdType.MESH
F32 = jnp.float32
BF16 = jnp.bfloat16
I32 = jnp.int32
I16 = jnp.int16

BLOCK_ROW = 16
SIDE = 16
SLOT = 64
CELLS = 1024
HALO = 256
FIELDS = 9
LEVELS = 55
PITCH = 56
ROWS = 512
CHUNKS = 2
CHUNK = ROWS // CHUNKS
EDGES = 3232
GROUPS = -(-EDGES // 128)
CORNER_A = CELLS + 192
CORNER_B = CELLS + 224


def dot(a, b):
    return jnp.dot(a, b, preferred_element_type=F32)


def split(x):
    high = x.astype(BF16)
    return high, (x - high.astype(F32)).astype(BF16)


def lanes(shape):
    return lax.broadcasted_iota(I32, shape, 1)


def rows_of(shape):
    return lax.broadcasted_iota(I32, shape, 0)


def kernel(
    field,
    area_in,
    dv_in,
    dc_in,
    ends_in,
    beside_in,
    send_in,
    acc,
    halo_h,
    halo_l,
    rim_h,
    rim_l,
    area,
    dv,
    dc,
    ends,
    beside,
    send,
    xf,
    xh,
    xl,
    select,
    lh,
    ll,
    near,
    coef_h,
    coef_l,
    diag,
    send_up,
    send_down,
    send_right,
    send_left,
    send_corner,
    got_up,
    got_down,
    got_right,
    got_left,
    got_corner,
    load_sem,
    send_sem,
    recv_sem,
):
    count = lax.axis_size("cells")
    me = lax.axis_index("cells")

    def at(offset):
        return lax.rem(me + (offset + count), count)

    offsets = (1, -1, BLOCK_ROW, -BLOCK_ROW, BLOCK_ROW - 1, 1 - BLOCK_ROW)
    barrier = pltpu.get_barrier_semaphore()
    for offset in offsets:
        pl.semaphore_signal(barrier, inc=1, device_id=(at(offset),), device_id_type=MESH)

    def load(i, src, dst):
        copy = pltpu.make_async_copy(src, dst, load_sem.at[i])
        copy.start()
        return copy

    list_load = load(FIELDS, send_in, send)
    loads = [load(f, field.at[f], xf.at[f]) for f in range(FIELDS)]
    table_loads = [
        load(FIELDS + 1 + i, src, dst)
        for i, (src, dst) in enumerate(
            ((beside_in, beside), (ends_in, ends), (dv_in, dv), (dc_in, dc), (area_in, area))
        )
    ]

    list_load.wait()
    lists = send[...]
    wide = (1, 128)
    lane1 = lanes(wide)
    first_cols = jnp.concatenate([lists[2:3], lists[3:4]], axis=1)
    second_cols = jnp.concatenate([lists[0:1], lists[1:2]], axis=1)
    near_cols = jnp.where(lane1 < 16, second_cols, pltpu.roll(second_cols, 80, 1))
    corner_cols = jnp.where(
        lane1 < 96,
        jnp.broadcast_to(lists[4:5, 0:1], wide),
        jnp.broadcast_to(lists[5:6, 0:1], wide),
    )
    second_cols = jnp.where(lane1 < 32, near_cols, jnp.where(lane1 < 64, -1, corner_cols))
    columns = jnp.concatenate([first_cols, second_cols], axis=1)

    def fill_select(i, carry):
        at_row = pl.multiple_of(i * 16, 16)
        ids = rows_of((16, HALO)) + at_row
        select[pl.ds(at_row, 16), :] = jnp.where(ids == columns, 1.0, 0.0).astype(BF16)
        return carry

    lax.fori_loop(0, CELLS // 16, fill_select, 0, unroll=8)

    half = CHUNK // 2
    part = CHUNK // 8
    corner_rows = CHUNK // 32

    def exchange(k, h):
        here = pl.ds(h * CHUNK, CHUNK)
        picked = dot(xh[here, :], select[...]) + dot(xl[here, :], select[...])
        lane = lanes((half, 128))
        top = picked[:half, :128]
        low_half = picked[half:, :128]
        send_up[k, h] = jnp.where(lane < 64, top, pltpu.roll(low_half, 64, 1))
        send_down[k, h] = jnp.where(lane < 64, pltpu.roll(top, 64, 1), low_half)
        rest = picked[:, 128:]
        group = lanes((part, 128)) // 16
        right = rest[0:part]
        left = pltpu.roll(rest[0:part], 112, 1)
        for g in range(1, 8):
            piece = rest[part * g : part * g + part]
            right = jnp.where(group == g, pltpu.roll(piece, 16 * g, 1), right)
            left = jnp.where(group == g, piece if g == 1 else pltpu.roll(piece, 16 * g - 16, 1), left)
        send_right[k, h] = right
        send_left[k, h] = left
        lane32 = lanes((32, 128))
        own = (lane32 >= 64) & ((lane32 & 31) == rows_of((32, 128)))
        folded = [
            jnp.sum(jnp.where(own, rest[32 * g : 32 * g + 32], 0.0), axis=0, keepdims=True)
            for g in range(corner_rows)
        ]
        send_corner[k, h] = jnp.concatenate(folded, axis=0)
        if k == 0 and h == 0:
            pl.semaphore_wait(barrier, 6)
        plan = (
            (send_up, got_up.at[k, h], offsets[2]),
            (send_down, got_down.at[k, h], offsets[3]),
            (send_right, got_right.at[k, h], offsets[0]),
            (send_left, got_left.at[k, h], offsets[1]),
            (send_corner, got_corner.at[k, h, 0], offsets[4]),
            (send_corner, got_corner.at[k, h, 1], offsets[5]),
        )
        copies = []
        for i, (src, dst, offset) in enumerate(plan):
            copies.append(
                pltpu.make_async_remote_copy(
                    src_ref=src.at[k, h],
                    dst_ref=dst,
                    send_sem=send_sem.at[k, h, i],
                    recv_sem=recv_sem.at[k, h, i],
                    device_id=(at(offset),),
                    device_id_type=MESH,
                )
            )
            copies[-1].start()
        return copies

    def receive(k, h, copies):
        for copy in copies:
            copy.wait_recv()
        lane = lanes((half, 128))
        up = got_up[k, h]
        down = got_down[k, h]
        halo_top = jnp.where(lane < 64, up, pltpu.roll(down, 64, 1))
        halo_low = jnp.where(lane < 64, pltpu.roll(up, 64, 1), down)
        for piece, start in ((halo_top, 0), (halo_low, half)):
            high, low = split(piece)
            halo_h[pl.ds(h * CHUNK + start, half), 0:128] = high
            halo_l[pl.ds(h * CHUNK + start, half), 0:128] = low
        right = got_right[k, h]
        left = got_left[k, h]
        corner_a = got_corner[k, h, 0]
        corner_b = got_corner[k, h, 1]
        shape = (part, 128)
        lane = lanes(shape)
        per_row = 32 // part
        corners = jnp.where(lanes((corner_rows, 128)) < 96, corner_a, corner_b)
        for g in range(8):
            row = g // per_row
            own = (lane & 31) == rows_of(shape) + part * (g % per_row)
            spread = jnp.where(own, jnp.broadcast_to(corners[row : row + 1], shape), 0.0)
            from_left = right if g == 0 else pltpu.roll(right, 128 - 16 * g, 1)
            from_right = left if g == 1 else pltpu.roll(left, (144 - 16 * g) % 128, 1)
            piece = jnp.where(
                lane < 16,
                from_left,
                jnp.where(lane < 32, from_right, jnp.where(lane < 64, 0.0, spread)),
            )
            high, low = split(piece)
            halo_h[pl.ds(h * CHUNK + part * g, part), 128:256] = high
            halo_l[pl.ds(h * CHUNK + part * g, part), 128:256] = low

    pad = jnp.zeros((PITCH - LEVELS, CELLS), F32)
    acc[FIELDS * PITCH : ROWS, :] = jnp.zeros((ROWS - FIELDS * PITCH, CELLS), F32)
    copies_a = []
    waited = 0
    for h in range(CHUNKS):
        while waited < FIELDS and waited * PITCH < (h + 1) * CHUNK:
            loads[waited].wait()
            acc[pl.ds(waited * PITCH, PITCH), :] = jnp.concatenate([xf[waited], pad], axis=0)
            waited += 1
        here = pl.ds(h * CHUNK, CHUNK)
        high, low = split(acc[here, :])
        xh[here, :] = high
        xl[here, :] = low
        copies_a.append(exchange(0, h))

    for copy in table_loads:
        copy.wait()
    packed = []
    weights = []
    for r in range(GROUPS):
        width = min(128, EDGES - 128 * r)
        where = slice(128 * r, 128 * r + width)
        both = ends[0:1, where] | (ends[1:2, where] << 11)
        ratio = (dv[where] / dc[where]).reshape(1, width)
        if width < 128:
            both = jnp.concatenate([both, jnp.zeros((1, 128 - width), I32)], axis=1)
            ratio = jnp.concatenate([ratio, jnp.zeros((1, 128 - width), F32)], axis=1)
        packed.append(jnp.broadcast_to(both, (8, 128)))
        weights.append(jnp.broadcast_to(ratio, (8, 128)))
    edge_ids = jnp.concatenate([beside[...], jnp.zeros((2, CELLS), I32)], axis=0)
    tile = (8, 128)
    valid = rows_of(tile) < 6
    for t in range(CELLS // 128):
        cols = slice(128 * t, 128 * t + 128)
        ids = edge_ids[:, cols]
        group = ids >> 7
        within = ids & 127
        both = jnp.zeros(tile, I32)
        ratio = jnp.zeros(tile, F32)
        for r in range(GROUPS):
            here = group == r
            both = jnp.where(here, jnp.take_along_axis(packed[r], within, axis=1), both)
            ratio = jnp.where(here, jnp.take_along_axis(weights[r], within, axis=1), ratio)
        end0 = both & 2047
        end1 = both >> 11
        other = jnp.where(end0 == lanes(tile) + 128 * t, end1, end0)
        beyond = other - CELLS
        slot = beyond >> 6
        place = beyond & 63
        start = jnp.where(
            slot == 2,
            CELLS,
            jnp.where(
                slot == 3,
                CELLS + 64,
                jnp.where(
                    slot == 0,
                    CELLS + 128,
                    jnp.where(slot == 1, CELLS + 144, jnp.where(slot == 4, CORNER_A, CORNER_B)),
                ),
            ),
        )
        other = jnp.where(other < CELLS, other, start + place)
        near[:, cols] = jnp.where(valid, other, -1)
        factor = jnp.where(valid, ratio / area[cols].reshape(1, 128), 0.0)
        high, low = (piece.astype(F32) for piece in split(factor))
        coef_h[:, cols] = high
        coef_l[:, cols] = low
        diag[0:1, cols] = jnp.sum(high + low, axis=0, keepdims=True)

    block = (16, 128)
    for t in range(CELLS // 128):
        cols = slice(128 * t, 128 * t + 128)
        nears = [jnp.broadcast_to(near[j : j + 1, cols], block).astype(I16) for j in range(6)]
        highs = [jnp.broadcast_to(coef_h[j : j + 1, cols], block).astype(BF16) for j in range(6)]
        lows = [jnp.broadcast_to(coef_l[j : j + 1, cols], block).astype(BF16) for j in range(6)]

        def put(high_ref, low_ref, at_row, ids, cols=cols, nears=nears, highs=highs, lows=lows):
            high = jnp.zeros(block, BF16)
            low = jnp.zeros(block, BF16)
            for j in range(6):
                here = ids == nears[j]
                high = jnp.where(here, highs[j], high)
                low = jnp.where(here, lows[j], low)
            high_ref[pl.ds(at_row, 16), cols] = high
            low_ref[pl.ds(at_row, 16), cols] = low

        def fill(i, ids, put=put):
            put(lh, ll, pl.multiple_of(i * 16, 16), ids)
            return ids + jnp.full(block, 16, I16)

        ids = lax.fori_loop(0, CELLS // 16, fill, rows_of(block).astype(I16), unroll=8)
        for at_row in range(0, HALO, 16):
            if CELLS + at_row >= CORNER_A:
                corner = CORNER_A if CELLS + at_row < CORNER_B else CORNER_B
                ids = jnp.full(block, corner, I16)
            put(rim_h, rim_l, at_row, ids)
            ids = ids + jnp.full(block, 16, I16)

    tiles = [slice(256 * n, 256 * n + 256) for n in range(CELLS // 256)]

    def own_part():
        for cols in tiles:
            a = dot(xh[...], lh[:, cols])
            a += dot(xh[...], ll[:, cols])
            a += dot(xl[...], lh[:, cols])
            acc[:, cols] = a - diag[0:1, cols] * acc[:, cols]

    def halo_part(h, then=None):
        here = pl.ds(h * CHUNK, CHUNK)
        for cols in tiles:
            a = dot(halo_h[here, :], rim_h[:, cols])
            a += dot(halo_h[here, :], rim_l[:, cols])
            a += dot(halo_l[here, :], rim_h[:, cols])
            value = acc[here, cols] + a
            acc[here, cols] = value
            if then is not None:
                then(here, cols, value)

    def keep(here, cols, value):
        high, low = split(value)
        xh[here, cols] = high
        xl[here, cols] = low

    own_part()
    copies_b = []
    for h in range(CHUNKS):
        receive(0, h, copies_a[h])
        halo_part(h, keep)
        copies_b.append(exchange(1, h))
    own_part()
    for h in range(CHUNKS):
        receive(1, h, copies_b[h])
        if h < CHUNKS - 1:
            halo_part(h)
    for h in range(CHUNKS):
        for copy in copies_a[h] + copies_b[h]:
            copy.wait_send()


def finish(acc, halo_h, halo_l, rim_h, rim_l, level, out, result, sem):
    spread = jnp.broadcast_to(level[...], (LEVELS, LEVELS))
    on_diagonal = lanes((LEVELS, LEVELS)) == rows_of((LEVELS, LEVELS))
    scale = -jnp.sum(jnp.where(on_diagonal, spread, 0.0), axis=1, keepdims=True)
    last = (CHUNKS - 1) * CHUNK
    copies = []

    def put(f):
        copies.append(pltpu.make_async_copy(result.at[f], out.at[f], sem.at[f]))
        copies[-1].start()

    for f in range(FIELDS):
        start = f * PITCH
        ready = min(LEVELS, max(0, last - start))
        if ready:
            result[f, 0:ready, :] = acc[start : start + ready, :] * scale[0:ready]
        if ready == LEVELS:
            put(f)
    tail = pl.ds(last, CHUNK)
    for n in range(CELLS // 256):
        cols = slice(256 * n, 256 * n + 256)
        a = dot(halo_h[tail, :], rim_h[:, cols])
        a += dot(halo_h[tail, :], rim_l[:, cols])
        a += dot(halo_l[tail, :], rim_h[:, cols])
        value = acc[tail, cols] + a
        for f in range(FIELDS):
            start = f * PITCH
            ready = min(LEVELS, max(0, last - start))
            if ready < LEVELS:
                result[f, ready:LEVELS, cols] = (
                    value[start + ready - last : start + LEVELS - last] * scale[ready:LEVELS]
                )
    for f in range(FIELDS):
        if last - f * PITCH < LEVELS:
            put(f)
    for copy in copies:
        copy.wait()


def shards(
    field, cell_area, dv_edge, dc_edge, cells_on_edge, edges_on_cell, send_cells, level_coef
):
    vmem = pl.BlockSpec(memory_space=pltpu.VMEM)
    hbm = pl.BlockSpec(memory_space=pltpu.HBM)
    half = CHUNK // 2
    part = CHUNK // 8
    corner_rows = CHUNK // 32
    ends = (2, CHUNKS)
    parts = pl.pallas_call(
        kernel,
        out_shape=[
            jax.ShapeDtypeStruct((ROWS, CELLS), F32),
            jax.ShapeDtypeStruct((ROWS, HALO), BF16),
            jax.ShapeDtypeStruct((ROWS, HALO), BF16),
            jax.ShapeDtypeStruct((HALO, CELLS), BF16),
            jax.ShapeDtypeStruct((HALO, CELLS), BF16),
        ],
        in_specs=[hbm] * 7,
        out_specs=[vmem] * 5,
        scratch_shapes=[
            pltpu.VMEM((CELLS,), F32),
            pltpu.VMEM((EDGES,), F32),
            pltpu.VMEM((EDGES,), F32),
            pltpu.VMEM((2, EDGES), I32),
            pltpu.VMEM((6, CELLS), I32),
            pltpu.VMEM((6, SLOT), I32),
            pltpu.VMEM((FIELDS, LEVELS, CELLS), F32),
            pltpu.VMEM((ROWS, CELLS), BF16),
            pltpu.VMEM((ROWS, CELLS), BF16),
            pltpu.VMEM((CELLS, HALO), BF16),
            pltpu.VMEM((CELLS, CELLS), BF16),
            pltpu.VMEM((CELLS, CELLS), BF16),
            pltpu.VMEM((8, CELLS), I32),
            pltpu.VMEM((8, CELLS), F32),
            pltpu.VMEM((8, CELLS), F32),
            pltpu.VMEM((1, CELLS), F32),
            pltpu.VMEM((*ends, half, 128), F32),
            pltpu.VMEM((*ends, half, 128), F32),
            pltpu.VMEM((*ends, part, 128), F32),
            pltpu.VMEM((*ends, part, 128), F32),
            pltpu.VMEM((*ends, corner_rows, 128), F32),
            pltpu.VMEM((*ends, half, 128), F32),
            pltpu.VMEM((*ends, half, 128), F32),
            pltpu.VMEM((*ends, part, 128), F32),
            pltpu.VMEM((*ends, part, 128), F32),
            pltpu.VMEM((*ends, 2, corner_rows, 128), F32),
            pltpu.SemaphoreType.DMA((FIELDS + 6,)),
            pltpu.SemaphoreType.DMA((*ends, 6)),
            pltpu.SemaphoreType.DMA((*ends, 6)),
        ],
        compiler_params=pltpu.CompilerParams(
            collective_id=0, has_side_effects=True, vmem_limit_bytes=40 * 1024 * 1024
        ),
        name="diffusion",
    )(
        *(
            pltpu.with_memory_space_constraint(x, pltpu.HBM)
            for x in (
                field, cell_area, dv_edge, dc_edge, cells_on_edge, edges_on_cell, send_cells
            )
        )
    )
    return pl.pallas_call(
        finish,
        out_shape=jax.ShapeDtypeStruct(field.shape, F32),
        in_specs=[vmem] * 6,
        out_specs=hbm,
        scratch_shapes=[
            pltpu.VMEM((FIELDS, LEVELS, CELLS), F32),
            pltpu.SemaphoreType.DMA((FIELDS,)),
        ],
        compiler_params=pltpu.CompilerParams(vmem_limit_bytes=40 * 1024 * 1024),
        name="finish",
    )(*parts, level_coef.reshape(1, -1))


def solution(mesh):
    return jax.shard_map(
        shards,
        mesh=mesh,
        in_specs=(
            P(None, None, "cells"),
            P("cells"),
            P("cells"),
            P("cells"),
            P(None, "cells"),
            P(None, "cells"),
            P(None, "cells"),
            P(),
        ),
        out_specs=P(None, None, "cells"),
        check_vma=False,
    )
```

```python
import functools

import jax
import jax.numpy as jnp
from jax import lax
from jax.experimental import pallas as pl
from jax.experimental.pallas import tpu as pltpu
from jax.sharding import PartitionSpec as P

MESH = pl.DeviceIdType.MESH
F32 = jnp.float32
BF16 = jnp.bfloat16
I32 = jnp.int32
I16 = jnp.int16

BLOCK_ROW = 16
SIDE = 16
SLOT = 64
CELLS = 1024
HALO = 256
FIELDS = 9
LEVELS = 55
PITCH = 56
ROWS = 512
CHUNKS = 2
CHUNK = ROWS // CHUNKS
EDGES = 3232
GROUPS = -(-EDGES // 128)
CORNER_A = CELLS + 192
CORNER_B = CELLS + 224


def dot(a, b):
    return jnp.dot(a, b, preferred_element_type=F32)


def split(x):
    high = x.astype(BF16)
    return high, (x - high.astype(F32)).astype(BF16)


def lanes(shape):
    return lax.broadcasted_iota(I32, shape, 1)


def rows_of(shape):
    return lax.broadcasted_iota(I32, shape, 0)


def kernel(
    field,
    area_in,
    dv_in,
    dc_in,
    ends_in,
    beside_in,
    send_in,
    acc,
    halo_h,
    halo_l,
    rim_h,
    rim_l,
    area,
    dv,
    dc,
    ends,
    beside,
    send,
    xf,
    xh,
    xl,
    select,
    lh,
    ll,
    near,
    coef_h,
    coef_l,
    diag,
    send_up,
    send_down,
    send_right,
    send_left,
    send_corner,
    got_up,
    got_down,
    got_right,
    got_left,
    got_corner,
    load_sem,
    send_sem,
    recv_sem,
):
    count = lax.axis_size("cells")
    me = lax.axis_index("cells")

    def at(offset):
        return lax.rem(me + (offset + count), count)

    offsets = (1, -1, BLOCK_ROW, -BLOCK_ROW, BLOCK_ROW - 1, 1 - BLOCK_ROW)
    barrier = pltpu.get_barrier_semaphore()
    for offset in offsets:
        pl.semaphore_signal(barrier, inc=1, device_id=(at(offset),), device_id_type=MESH)

    def load(i, src, dst):
        copy = pltpu.make_async_copy(src, dst, load_sem.at[i])
        copy.start()
        return copy

    list_load = load(FIELDS, send_in, send)
    loads = [load(f, field.at[f], xf.at[f]) for f in range(FIELDS)]
    table_loads = [
        load(FIELDS + 1 + i, src, dst)
        for i, (src, dst) in enumerate(
            ((beside_in, beside), (ends_in, ends), (dv_in, dv), (dc_in, dc), (area_in, area))
        )
    ]

    list_load.wait()
    lists = send[...]
    wide = (1, 128)
    lane1 = lanes(wide)
    first_cols = jnp.concatenate([lists[2:3], lists[3:4]], axis=1)
    second_cols = jnp.concatenate([lists[0:1], lists[1:2]], axis=1)
    near_cols = jnp.where(lane1 < 16, second_cols, pltpu.roll(second_cols, 80, 1))
    corner_cols = jnp.where(
        lane1 < 96,
        jnp.broadcast_to(lists[4:5, 0:1], wide),
        jnp.broadcast_to(lists[5:6, 0:1], wide),
    )
    second_cols = jnp.where(lane1 < 32, near_cols, jnp.where(lane1 < 64, -1, corner_cols))
    columns = jnp.concatenate([first_cols, second_cols], axis=1)

    def fill_select(i, carry):
        at_row = pl.multiple_of(i * 16, 16)
        ids = rows_of((16, HALO)) + at_row
        select[pl.ds(at_row, 16), :] = jnp.where(ids == columns, 1.0, 0.0).astype(BF16)
        return carry

    lax.fori_loop(0, CELLS // 16, fill_select, 0, unroll=8)

    half = CHUNK // 2
    part = CHUNK // 8
    corner_rows = CHUNK // 32

    def exchange(k, h):
        here = pl.ds(h * CHUNK, CHUNK)
        picked = dot(xh[here, :], select[...]) + dot(xl[here, :], select[...])
        copies = []

        def start(i, src, dst, offset):
            copies.append(
                pltpu.make_async_remote_copy(
                    src_ref=src.at[k, h],
                    dst_ref=dst,
                    send_sem=send_sem.at[k, h, i],
                    recv_sem=recv_sem.at[k, h, i],
                    device_id=(at(offset),),
                    device_id_type=MESH,
                )
            )
            copies[-1].start()

        rest = picked[:, 128:]
        lane32 = lanes((32, 128))
        own = (lane32 >= 64) & ((lane32 & 31) == rows_of((32, 128)))
        folded = [
            jnp.sum(jnp.where(own, rest[32 * g : 32 * g + 32], 0.0), axis=0, keepdims=True)
            for g in range(corner_rows)
        ]
        send_corner[k, h] = jnp.concatenate(folded, axis=0)
        lane = lanes((half, 128))
        top = picked[:half, :128]
        low_half = picked[half:, :128]
        send_up[k, h] = jnp.where(lane < 64, top, pltpu.roll(low_half, 64, 1))
        send_down[k, h] = jnp.where(lane < 64, pltpu.roll(top, 64, 1), low_half)
        if k == 0 and h == 0:
            pl.semaphore_wait(barrier, 6)
        start(4, send_corner, got_corner.at[k, h, 0], offsets[4])
        start(5, send_corner, got_corner.at[k, h, 1], offsets[5])
        start(2, send_up, got_up.at[k, h], offsets[2])
        start(3, send_down, got_down.at[k, h], offsets[3])
        group = lanes((part, 128)) // 16
        right = rest[0:part]
        left = pltpu.roll(rest[0:part], 112, 1)
        for g in range(1, 8):
            piece = rest[part * g : part * g + part]
            right = jnp.where(group == g, pltpu.roll(piece, 16 * g, 1), right)
            left = jnp.where(group == g, piece if g == 1 else pltpu.roll(piece, 16 * g - 16, 1), left)
        send_right[k, h] = right
        send_left[k, h] = left
        start(0, send_right, got_right.at[k, h], offsets[0])
        start(1, send_left, got_left.at[k, h], offsets[1])
        return copies

    def receive(k, h, copies):
        for copy in copies:
            copy.wait_recv()
        lane = lanes((half, 128))
        up = got_up[k, h]
        down = got_down[k, h]
        halo_top = jnp.where(lane < 64, up, pltpu.roll(down, 64, 1))
        halo_low = jnp.where(lane < 64, pltpu.roll(up, 64, 1), down)
        for piece, start in ((halo_top, 0), (halo_low, half)):
            high, low = split(piece)
            halo_h[pl.ds(h * CHUNK + start, half), 0:128] = high
            halo_l[pl.ds(h * CHUNK + start, half), 0:128] = low
        right = got_right[k, h]
        left = got_left[k, h]
        corner_a = got_corner[k, h, 0]
        corner_b = got_corner[k, h, 1]
        shape = (part, 128)
        lane = lanes(shape)
        per_row = 32 // part
        corners = jnp.where(lanes((corner_rows, 128)) < 96, corner_a, corner_b)
        for g in range(8):
            row = g // per_row
            own = (lane & 31) == rows_of(shape) + part * (g % per_row)
            spread = jnp.where(own, jnp.broadcast_to(corners[row : row + 1], shape), 0.0)
            from_left = right if g == 0 else pltpu.roll(right, 128 - 16 * g, 1)
            from_right = left if g == 1 else pltpu.roll(left, (144 - 16 * g) % 128, 1)
            piece = jnp.where(
                lane < 16,
                from_left,
                jnp.where(lane < 32, from_right, jnp.where(lane < 64, 0.0, spread)),
            )
            high, low = split(piece)
            halo_h[pl.ds(h * CHUNK + part * g, part), 128:256] = high
            halo_l[pl.ds(h * CHUNK + part * g, part), 128:256] = low

    pad = jnp.zeros((PITCH - LEVELS, CELLS), F32)
    acc[FIELDS * PITCH : ROWS, :] = jnp.zeros((ROWS - FIELDS * PITCH, CELLS), F32)
    copies_a = []
    waited = 0
    for h in range(CHUNKS):
        while waited < FIELDS and waited * PITCH < (h + 1) * CHUNK:
            loads[waited].wait()
            acc[pl.ds(waited * PITCH, PITCH), :] = jnp.concatenate([xf[waited], pad], axis=0)
            waited += 1
        here = pl.ds(h * CHUNK, CHUNK)
        high, low = split(acc[here, :])
        xh[here, :] = high
        xl[here, :] = low
        copies_a.append(exchange(0, h))

    for copy in table_loads:
        copy.wait()
    packed = []
    weights = []
    for r in range(GROUPS):
        width = min(128, EDGES - 128 * r)
        where = slice(128 * r, 128 * r + width)
        both = ends[0:1, where] | (ends[1:2, where] << 11)
        ratio = (dv[where] / dc[where]).reshape(1, width)
        if width < 128:
            both = jnp.concatenate([both, jnp.zeros((1, 128 - width), I32)], axis=1)
            ratio = jnp.concatenate([ratio, jnp.zeros((1, 128 - width), F32)], axis=1)
        packed.append(jnp.broadcast_to(both, (8, 128)))
        weights.append(jnp.broadcast_to(ratio, (8, 128)))
    edge_ids = jnp.concatenate([beside[...], jnp.zeros((2, CELLS), I32)], axis=0)
    tile = (8, 128)
    valid = rows_of(tile) < 6
    for t in range(CELLS // 128):
        cols = slice(128 * t, 128 * t + 128)
        ids = edge_ids[:, cols]
        group = ids >> 7
        within = ids & 127
        both = jnp.zeros(tile, I32)
        ratio = jnp.zeros(tile, F32)
        for r in range(GROUPS):
            here = group == r
            both = jnp.where(here, jnp.take_along_axis(packed[r], within, axis=1), both)
            ratio = jnp.where(here, jnp.take_along_axis(weights[r], within, axis=1), ratio)
        end0 = both & 2047
        end1 = both >> 11
        other = jnp.where(end0 == lanes(tile) + 128 * t, end1, end0)
        beyond = other - CELLS
        slot = beyond >> 6
        place = beyond & 63
        start = jnp.where(
            slot == 2,
            CELLS,
            jnp.where(
                slot == 3,
                CELLS + 64,
                jnp.where(
                    slot == 0,
                    CELLS + 128,
                    jnp.where(slot == 1, CELLS + 144, jnp.where(slot == 4, CORNER_A, CORNER_B)),
                ),
            ),
        )
        other = jnp.where(other < CELLS, other, start + place)
        near[:, cols] = jnp.where(valid, other, -1)
        factor = jnp.where(valid, ratio / area[cols].reshape(1, 128), 0.0)
        high, low = (piece.astype(F32) for piece in split(factor))
        coef_h[:, cols] = high
        coef_l[:, cols] = low
        diag[0:1, cols] = jnp.sum(high + low, axis=0, keepdims=True)

    block = (16, 128)
    for t in range(CELLS // 128):
        cols = slice(128 * t, 128 * t + 128)
        nears = [jnp.broadcast_to(near[j : j + 1, cols], block).astype(I16) for j in range(6)]
        highs = [jnp.broadcast_to(coef_h[j : j + 1, cols], block).astype(BF16) for j in range(6)]
        lows = [jnp.broadcast_to(coef_l[j : j + 1, cols], block).astype(BF16) for j in range(6)]

        def put(high_ref, low_ref, at_row, ids, cols=cols, nears=nears, highs=highs, lows=lows):
            high = jnp.zeros(block, BF16)
            low = jnp.zeros(block, BF16)
            for j in range(6):
                here = ids == nears[j]
                high = jnp.where(here, highs[j], high)
                low = jnp.where(here, lows[j], low)
            high_ref[pl.ds(at_row, 16), cols] = high
            low_ref[pl.ds(at_row, 16), cols] = low

        def fill(i, ids, put=put):
            put(lh, ll, pl.multiple_of(i * 16, 16), ids)
            return ids + jnp.full(block, 16, I16)

        ids = lax.fori_loop(0, CELLS // 16, fill, rows_of(block).astype(I16), unroll=8)
        for at_row in range(0, HALO, 16):
            if CELLS + at_row >= CORNER_A:
                corner = CORNER_A if CELLS + at_row < CORNER_B else CORNER_B
                ids = jnp.full(block, corner, I16)
            put(rim_h, rim_l, at_row, ids)
            ids = ids + jnp.full(block, 16, I16)

    tiles = [slice(256 * n, 256 * n + 256) for n in range(CELLS // 256)]

    def own_part():
        for cols in tiles:
            a = dot(xh[...], lh[:, cols])
            a += dot(xh[...], ll[:, cols])
            a += dot(xl[...], lh[:, cols])
            acc[:, cols] = a - diag[0:1, cols] * acc[:, cols]

    def halo_part(h, then=None):
        here = pl.ds(h * CHUNK, CHUNK)
        for cols in tiles:
            a = dot(halo_h[here, :], rim_h[:, cols])
            a += dot(halo_h[here, :], rim_l[:, cols])
            a += dot(halo_l[here, :], rim_h[:, cols])
            value = acc[here, cols] + a
            acc[here, cols] = value
            if then is not None:
                then(here, cols, value)

    def keep(here, cols, value):
        high, low = split(value)
        xh[here, cols] = high
        xl[here, cols] = low

    own_part()
    copies_b = []
    for h in range(CHUNKS):
        receive(0, h, copies_a[h])
        halo_part(h, keep)
        copies_b.append(exchange(1, h))
    own_part()
    for h in range(CHUNKS):
        receive(1, h, copies_b[h])
        if h < CHUNKS - 1:
            halo_part(h)
    for h in range(CHUNKS):
        for copy in copies_a[h] + copies_b[h]:
            copy.wait_send()


def finish(acc, halo_h, halo_l, rim_h, rim_l, level, out, result, sem):
    spread = jnp.broadcast_to(level[...], (LEVELS, LEVELS))
    on_diagonal = lanes((LEVELS, LEVELS)) == rows_of((LEVELS, LEVELS))
    scale = -jnp.sum(jnp.where(on_diagonal, spread, 0.0), axis=1, keepdims=True)
    last = (CHUNKS - 1) * CHUNK
    copies = []

    def put(f):
        copies.append(pltpu.make_async_copy(result.at[f], out.at[f], sem.at[f]))
        copies[-1].start()

    for f in range(FIELDS):
        start = f * PITCH
        ready = min(LEVELS, max(0, last - start))
        if ready:
            result[f, 0:ready, :] = acc[start : start + ready, :] * scale[0:ready]
        if ready == LEVELS:
            put(f)
    tail = pl.ds(last, CHUNK)
    for n in range(CELLS // 256):
        cols = slice(256 * n, 256 * n + 256)
        a = dot(halo_h[tail, :], rim_h[:, cols])
        a += dot(halo_h[tail, :], rim_l[:, cols])
        a += dot(halo_l[tail, :], rim_h[:, cols])
        value = acc[tail, cols] + a
        for f in range(FIELDS):
            start = f * PITCH
            ready = min(LEVELS, max(0, last - start))
            if ready < LEVELS:
                result[f, ready:LEVELS, cols] = (
                    value[start + ready - last : start + LEVELS - last] * scale[ready:LEVELS]
                )
    for f in range(FIELDS):
        if last - f * PITCH < LEVELS:
            put(f)
    for copy in copies:
        copy.wait()


def shards(
    field, cell_area, dv_edge, dc_edge, cells_on_edge, edges_on_cell, send_cells, level_coef
):
    vmem = pl.BlockSpec(memory_space=pltpu.VMEM)
    hbm = pl.BlockSpec(memory_space=pltpu.HBM)
    half = CHUNK // 2
    part = CHUNK // 8
    corner_rows = CHUNK // 32
    ends = (2, CHUNKS)
    parts = pl.pallas_call(
        kernel,
        out_shape=[
            jax.ShapeDtypeStruct((ROWS, CELLS), F32),
            jax.ShapeDtypeStruct((ROWS, HALO), BF16),
            jax.ShapeDtypeStruct((ROWS, HALO), BF16),
            jax.ShapeDtypeStruct((HALO, CELLS), BF16),
            jax.ShapeDtypeStruct((HALO, CELLS), BF16),
        ],
        in_specs=[hbm] * 7,
        out_specs=[vmem] * 5,
        scratch_shapes=[
            pltpu.VMEM((CELLS,), F32),
            pltpu.VMEM((EDGES,), F32),
            pltpu.VMEM((EDGES,), F32),
            pltpu.VMEM((2, EDGES), I32),
            pltpu.VMEM((6, CELLS), I32),
            pltpu.VMEM((6, SLOT), I32),
            pltpu.VMEM((FIELDS, LEVELS, CELLS), F32),
            pltpu.VMEM((ROWS, CELLS), BF16),
            pltpu.VMEM((ROWS, CELLS), BF16),
            pltpu.VMEM((CELLS, HALO), BF16),
            pltpu.VMEM((CELLS, CELLS), BF16),
            pltpu.VMEM((CELLS, CELLS), BF16),
            pltpu.VMEM((8, CELLS), I32),
            pltpu.VMEM((8, CELLS), F32),
            pltpu.VMEM((8, CELLS), F32),
            pltpu.VMEM((1, CELLS), F32),
            pltpu.VMEM((*ends, half, 128), F32),
            pltpu.VMEM((*ends, half, 128), F32),
            pltpu.VMEM((*ends, part, 128), F32),
            pltpu.VMEM((*ends, part, 128), F32),
            pltpu.VMEM((*ends, corner_rows, 128), F32),
            pltpu.VMEM((*ends, half, 128), F32),
            pltpu.VMEM((*ends, half, 128), F32),
            pltpu.VMEM((*ends, part, 128), F32),
            pltpu.VMEM((*ends, part, 128), F32),
            pltpu.VMEM((*ends, 2, corner_rows, 128), F32),
            pltpu.SemaphoreType.DMA((FIELDS + 6,)),
            pltpu.SemaphoreType.DMA((*ends, 6)),
            pltpu.SemaphoreType.DMA((*ends, 6)),
        ],
        compiler_params=pltpu.CompilerParams(
            collective_id=0, has_side_effects=True, vmem_limit_bytes=40 * 1024 * 1024
        ),
        name="diffusion",
    )(
        *(
            pltpu.with_memory_space_constraint(x, pltpu.HBM)
            for x in (
                field, cell_area, dv_edge, dc_edge, cells_on_edge, edges_on_cell, send_cells
            )
        )
    )
    return pl.pallas_call(
        finish,
        out_shape=jax.ShapeDtypeStruct(field.shape, F32),
        in_specs=[vmem] * 6,
        out_specs=hbm,
        scratch_shapes=[
            pltpu.VMEM((FIELDS, LEVELS, CELLS), F32),
            pltpu.SemaphoreType.DMA((FIELDS,)),
        ],
        compiler_params=pltpu.CompilerParams(vmem_limit_bytes=40 * 1024 * 1024),
        name="finish",
    )(*parts, level_coef.reshape(1, -1))


def solution(mesh):
    return jax.shard_map(
        shards,
        mesh=mesh,
        in_specs=(
            P(None, None, "cells"),
            P("cells"),
            P("cells"),
            P("cells"),
            P(None, "cells"),
            P(None, "cells"),
            P(None, "cells"),
            P(),
        ),
        out_specs=P(None, None, "cells"),
        check_vma=False,
    )
```

```python
import functools

import jax
import jax.numpy as jnp
from jax import lax
from jax.experimental import pallas as pl
from jax.experimental.pallas import tpu as pltpu
from jax.sharding import PartitionSpec as P

MESH = pl.DeviceIdType.MESH
F32 = jnp.float32
BF16 = jnp.bfloat16
I32 = jnp.int32
I16 = jnp.int16

BLOCK_ROW = 16
SIDE = 16
SLOT = 64
CELLS = 1024
HALO = 256
FIELDS = 9
LEVELS = 55
PITCH = 56
ROWS = 512
CHUNKS = 2
CHUNK = ROWS // CHUNKS
EDGES = 3232
GROUPS = -(-EDGES // 128)
CORNER_A = CELLS + 192
CORNER_B = CELLS + 224


def dot(a, b):
    return jnp.dot(a, b, preferred_element_type=F32)


def split(x):
    high = x.astype(BF16)
    return high, (x - high.astype(F32)).astype(BF16)


def lanes(shape):
    return lax.broadcasted_iota(I32, shape, 1)


def rows_of(shape):
    return lax.broadcasted_iota(I32, shape, 0)


def kernel(
    field,
    area_in,
    dv_in,
    dc_in,
    ends_in,
    beside_in,
    send_in,
    acc,
    halo_h,
    halo_l,
    rim_h,
    rim_l,
    area,
    dv,
    dc,
    ends,
    beside,
    send,
    xf,
    xh,
    xl,
    select,
    lh,
    ll,
    near,
    coef_h,
    coef_l,
    diag,
    send_up,
    send_down,
    send_right,
    send_left,
    send_corner,
    got_up,
    got_down,
    got_right,
    got_left,
    got_corner,
    load_sem,
    send_sem,
    recv_sem,
):
    count = lax.axis_size("cells")
    me = lax.axis_index("cells")

    def at(offset):
        return lax.rem(me + (offset + count), count)

    offsets = (1, -1, BLOCK_ROW, -BLOCK_ROW, BLOCK_ROW - 1, 1 - BLOCK_ROW)
    barrier = pltpu.get_barrier_semaphore()
    for offset in offsets:
        pl.semaphore_signal(barrier, inc=1, device_id=(at(offset),), device_id_type=MESH)

    def load(i, src, dst):
        copy = pltpu.make_async_copy(src, dst, load_sem.at[i])
        copy.start()
        return copy

    list_load = load(FIELDS, send_in, send)
    table_loads = [
        load(FIELDS + 1 + i, src, dst)
        for i, (src, dst) in enumerate(
            ((beside_in, beside), (ends_in, ends), (dv_in, dv), (dc_in, dc), (area_in, area))
        )
    ]

    loads = [load(f, field.at[f], xf.at[f]) for f in range(FIELDS)]

    list_load.wait()
    lists = send[...]
    wide = (1, 128)
    lane1 = lanes(wide)
    first_cols = jnp.concatenate([lists[2:3], lists[3:4]], axis=1)
    second_cols = jnp.concatenate([lists[0:1], lists[1:2]], axis=1)
    near_cols = jnp.where(lane1 < 16, second_cols, pltpu.roll(second_cols, 80, 1))
    corner_cols = jnp.where(
        lane1 < 96,
        jnp.broadcast_to(lists[4:5, 0:1], wide),
        jnp.broadcast_to(lists[5:6, 0:1], wide),
    )
    second_cols = jnp.where(lane1 < 32, near_cols, jnp.where(lane1 < 64, -1, corner_cols))
    columns = jnp.concatenate([first_cols, second_cols], axis=1)

    def fill_select(i, carry):
        at_row = pl.multiple_of(i * 16, 16)
        ids = rows_of((16, HALO)) + at_row
        select[pl.ds(at_row, 16), :] = jnp.where(ids == columns, 1.0, 0.0).astype(BF16)
        return carry

    lax.fori_loop(0, CELLS // 16, fill_select, 0, unroll=8)

    half = CHUNK // 2
    part = CHUNK // 8
    corner_rows = CHUNK // 32

    def exchange(k, h):
        here = pl.ds(h * CHUNK, CHUNK)
        picked = dot(xh[here, :], select[...]) + dot(xl[here, :], select[...])
        copies = []

        def start(i, src, dst, offset):
            copies.append(
                pltpu.make_async_remote_copy(
                    src_ref=src.at[k, h],
                    dst_ref=dst,
                    send_sem=send_sem.at[k, h, i],
                    recv_sem=recv_sem.at[k, h, i],
                    device_id=(at(offset),),
                    device_id_type=MESH,
                )
            )
            copies[-1].start()

        rest = picked[:, 128:]
        lane32 = lanes((32, 128))
        own = (lane32 >= 64) & ((lane32 & 31) == rows_of((32, 128)))
        folded = [
            jnp.sum(jnp.where(own, rest[32 * g : 32 * g + 32], 0.0), axis=0, keepdims=True)
            for g in range(corner_rows)
        ]
        send_corner[k, h] = jnp.concatenate(folded, axis=0)
        lane = lanes((half, 128))
        top = picked[:half, :128]
        low_half = picked[half:, :128]
        send_up[k, h] = jnp.where(lane < 64, top, pltpu.roll(low_half, 64, 1))
        send_down[k, h] = jnp.where(lane < 64, pltpu.roll(top, 64, 1), low_half)
        if k == 0 and h == 0:
            pl.semaphore_wait(barrier, 6)
        start(4, send_corner, got_corner.at[k, h, 0], offsets[4])
        start(5, send_corner, got_corner.at[k, h, 1], offsets[5])
        start(2, send_up, got_up.at[k, h], offsets[2])
        start(3, send_down, got_down.at[k, h], offsets[3])
        group = lanes((part, 128)) // 16
        right = rest[0:part]
        left = pltpu.roll(rest[0:part], 112, 1)
        for g in range(1, 8):
            piece = rest[part * g : part * g + part]
            right = jnp.where(group == g, pltpu.roll(piece, 16 * g, 1), right)
            left = jnp.where(group == g, piece if g == 1 else pltpu.roll(piece, 16 * g - 16, 1), left)
        send_right[k, h] = right
        send_left[k, h] = left
        start(0, send_right, got_right.at[k, h], offsets[0])
        start(1, send_left, got_left.at[k, h], offsets[1])
        return copies

    def receive(k, h, copies):
        for copy in copies:
            copy.wait_recv()
        lane = lanes((half, 128))
        up = got_up[k, h]
        down = got_down[k, h]
        halo_top = jnp.where(lane < 64, up, pltpu.roll(down, 64, 1))
        halo_low = jnp.where(lane < 64, pltpu.roll(up, 64, 1), down)
        for piece, start in ((halo_top, 0), (halo_low, half)):
            high, low = split(piece)
            halo_h[pl.ds(h * CHUNK + start, half), 0:128] = high
            halo_l[pl.ds(h * CHUNK + start, half), 0:128] = low
        right = got_right[k, h]
        left = got_left[k, h]
        corner_a = got_corner[k, h, 0]
        corner_b = got_corner[k, h, 1]
        shape = (part, 128)
        lane = lanes(shape)
        per_row = 32 // part
        corners = jnp.where(lanes((corner_rows, 128)) < 96, corner_a, corner_b)
        for g in range(8):
            row = g // per_row
            own = (lane & 31) == rows_of(shape) + part * (g % per_row)
            spread = jnp.where(own, jnp.broadcast_to(corners[row : row + 1], shape), 0.0)
            from_left = right if g == 0 else pltpu.roll(right, 128 - 16 * g, 1)
            from_right = left if g == 1 else pltpu.roll(left, (144 - 16 * g) % 128, 1)
            piece = jnp.where(
                lane < 16,
                from_left,
                jnp.where(lane < 32, from_right, jnp.where(lane < 64, 0.0, spread)),
            )
            high, low = split(piece)
            halo_h[pl.ds(h * CHUNK + part * g, part), 128:256] = high
            halo_l[pl.ds(h * CHUNK + part * g, part), 128:256] = low

    for copy in table_loads:
        copy.wait()
    packed = []
    weights = []
    for r in range(GROUPS):
        width = min(128, EDGES - 128 * r)
        where = slice(128 * r, 128 * r + width)
        both = ends[0:1, where] | (ends[1:2, where] << 11)
        ratio = (dv[where] / dc[where]).reshape(1, width)
        if width < 128:
            both = jnp.concatenate([both, jnp.zeros((1, 128 - width), I32)], axis=1)
            ratio = jnp.concatenate([ratio, jnp.zeros((1, 128 - width), F32)], axis=1)
        packed.append(jnp.broadcast_to(both, (8, 128)))
        weights.append(jnp.broadcast_to(ratio, (8, 128)))
    edge_ids = jnp.concatenate([beside[...], jnp.zeros((2, CELLS), I32)], axis=0)
    tile = (8, 128)
    valid = rows_of(tile) < 6
    for t in range(CELLS // 128):
        cols = slice(128 * t, 128 * t + 128)
        ids = edge_ids[:, cols]
        group = ids >> 7
        within = ids & 127
        both = jnp.zeros(tile, I32)
        ratio = jnp.zeros(tile, F32)
        for r in range(GROUPS):
            here = group == r
            both = jnp.where(here, jnp.take_along_axis(packed[r], within, axis=1), both)
            ratio = jnp.where(here, jnp.take_along_axis(weights[r], within, axis=1), ratio)
        end0 = both & 2047
        end1 = both >> 11
        other = jnp.where(end0 == lanes(tile) + 128 * t, end1, end0)
        beyond = other - CELLS
        slot = beyond >> 6
        place = beyond & 63
        start = jnp.where(
            slot == 2,
            CELLS,
            jnp.where(
                slot == 3,
                CELLS + 64,
                jnp.where(
                    slot == 0,
                    CELLS + 128,
                    jnp.where(slot == 1, CELLS + 144, jnp.where(slot == 4, CORNER_A, CORNER_B)),
                ),
            ),
        )
        other = jnp.where(other < CELLS, other, start + place)
        near[:, cols] = jnp.where(valid, other, -1)
        factor = jnp.where(valid, ratio / area[cols].reshape(1, 128), 0.0)
        high, low = (piece.astype(F32) for piece in split(factor))
        coef_h[:, cols] = high
        coef_l[:, cols] = low
        diag[0:1, cols] = jnp.sum(high + low, axis=0, keepdims=True)

    pad = jnp.zeros((PITCH - LEVELS, CELLS), F32)
    acc[FIELDS * PITCH : ROWS, :] = jnp.zeros((ROWS - FIELDS * PITCH, CELLS), F32)
    copies_a = []
    waited = 0
    for h in range(CHUNKS):
        while waited < FIELDS and waited * PITCH < (h + 1) * CHUNK:
            loads[waited].wait()
            acc[pl.ds(waited * PITCH, PITCH), :] = jnp.concatenate([xf[waited], pad], axis=0)
            waited += 1
        here = pl.ds(h * CHUNK, CHUNK)
        high, low = split(acc[here, :])
        xh[here, :] = high
        xl[here, :] = low
        copies_a.append(exchange(0, h))

    block = (16, 128)
    first_ids = rows_of(block).astype(I16)

    def build(t):
        cols = slice(128 * t, 128 * t + 128)
        nears = [jnp.broadcast_to(near[j : j + 1, cols], block).astype(I16) for j in range(6)]
        highs = [jnp.broadcast_to(coef_h[j : j + 1, cols], block).astype(BF16) for j in range(6)]
        lows = [jnp.broadcast_to(coef_l[j : j + 1, cols], block).astype(BF16) for j in range(6)]

        def put(high_ref, low_ref, at_row, ids):
            high = jnp.zeros(block, BF16)
            low = jnp.zeros(block, BF16)
            for j in range(6):
                here = ids == nears[j]
                high = jnp.where(here, highs[j], high)
                low = jnp.where(here, lows[j], low)
            high_ref[at_row : at_row + 16, cols] = high
            low_ref[at_row : at_row + 16, cols] = low

        for at_row in range(0, CELLS, 16):
            put(lh, ll, at_row, first_ids + jnp.full(block, at_row, I16))
        for at_row in range(0, HALO, 16):
            ids = first_ids + jnp.full(block, CELLS + at_row, I16)
            if CELLS + at_row >= CORNER_A:
                corner = CORNER_A if CELLS + at_row < CORNER_B else CORNER_B
                ids = jnp.full(block, corner, I16)
            put(rim_h, rim_l, at_row, ids)

    tiles = [slice(256 * n, 256 * n + 256) for n in range(CELLS // 256)]

    def own_part(building=False):
        for n, cols in enumerate(tiles):
            if building and n + 1 < len(tiles):
                build(2 * n + 2)
                build(2 * n + 3)
            a = dot(xh[...], lh[:, cols])
            a += dot(xh[...], ll[:, cols])
            a += dot(xl[...], lh[:, cols])
            acc[:, cols] = a - diag[0:1, cols] * acc[:, cols]

    def halo_part(h, then=None):
        here = pl.ds(h * CHUNK, CHUNK)
        for cols in tiles:
            a = dot(halo_h[here, :], rim_h[:, cols])
            a += dot(halo_h[here, :], rim_l[:, cols])
            a += dot(halo_l[here, :], rim_h[:, cols])
            value = acc[here, cols] + a
            acc[here, cols] = value
            if then is not None:
                then(here, cols, value)

    def keep(here, cols, value):
        high, low = split(value)
        xh[here, cols] = high
        xl[here, cols] = low

    build(0)
    build(1)
    own_part(building=True)
    copies_b = []
    for h in range(CHUNKS):
        receive(0, h, copies_a[h])
        halo_part(h, keep)
        copies_b.append(exchange(1, h))
    own_part()
    for h in range(CHUNKS):
        receive(1, h, copies_b[h])
        if h < CHUNKS - 1:
            halo_part(h)
    for h in range(CHUNKS):
        for copy in copies_a[h] + copies_b[h]:
            copy.wait_send()


def finish(acc, halo_h, halo_l, rim_h, rim_l, level, out, result, sem):
    spread = jnp.broadcast_to(level[...], (LEVELS, LEVELS))
    on_diagonal = lanes((LEVELS, LEVELS)) == rows_of((LEVELS, LEVELS))
    scale = -jnp.sum(jnp.where(on_diagonal, spread, 0.0), axis=1, keepdims=True)
    last = (CHUNKS - 1) * CHUNK
    copies = []

    def put(f):
        copies.append(pltpu.make_async_copy(result.at[f], out.at[f], sem.at[f]))
        copies[-1].start()

    for f in range(FIELDS):
        start = f * PITCH
        ready = min(LEVELS, max(0, last - start))
        if ready:
            result[f, 0:ready, :] = acc[start : start + ready, :] * scale[0:ready]
        if ready == LEVELS:
            put(f)
    tail = pl.ds(last, CHUNK)
    for n in range(CELLS // 256):
        cols = slice(256 * n, 256 * n + 256)
        a = dot(halo_h[tail, :], rim_h[:, cols])
        a += dot(halo_h[tail, :], rim_l[:, cols])
        a += dot(halo_l[tail, :], rim_h[:, cols])
        value = acc[tail, cols] + a
        for f in range(FIELDS):
            start = f * PITCH
            ready = min(LEVELS, max(0, last - start))
            if ready < LEVELS:
                result[f, ready:LEVELS, cols] = (
                    value[start + ready - last : start + LEVELS - last] * scale[ready:LEVELS]
                )
    for f in range(FIELDS):
        if last - f * PITCH < LEVELS:
            put(f)
    for copy in copies:
        copy.wait()


def shards(
    field, cell_area, dv_edge, dc_edge, cells_on_edge, edges_on_cell, send_cells, level_coef
):
    vmem = pl.BlockSpec(memory_space=pltpu.VMEM)
    hbm = pl.BlockSpec(memory_space=pltpu.HBM)
    half = CHUNK // 2
    part = CHUNK // 8
    corner_rows = CHUNK // 32
    ends = (2, CHUNKS)
    parts = pl.pallas_call(
        kernel,
        out_shape=[
            jax.ShapeDtypeStruct((ROWS, CELLS), F32),
            jax.ShapeDtypeStruct((ROWS, HALO), BF16),
            jax.ShapeDtypeStruct((ROWS, HALO), BF16),
            jax.ShapeDtypeStruct((HALO, CELLS), BF16),
            jax.ShapeDtypeStruct((HALO, CELLS), BF16),
        ],
        in_specs=[hbm] * 7,
        out_specs=[vmem] * 5,
        scratch_shapes=[
            pltpu.VMEM((CELLS,), F32),
            pltpu.VMEM((EDGES,), F32),
            pltpu.VMEM((EDGES,), F32),
            pltpu.VMEM((2, EDGES), I32),
            pltpu.VMEM((6, CELLS), I32),
            pltpu.VMEM((6, SLOT), I32),
            pltpu.VMEM((FIELDS, LEVELS, CELLS), F32),
            pltpu.VMEM((ROWS, CELLS), BF16),
            pltpu.VMEM((ROWS, CELLS), BF16),
            pltpu.VMEM((CELLS, HALO), BF16),
            pltpu.VMEM((CELLS, CELLS), BF16),
            pltpu.VMEM((CELLS, CELLS), BF16),
            pltpu.VMEM((8, CELLS), I32),
            pltpu.VMEM((8, CELLS), F32),
            pltpu.VMEM((8, CELLS), F32),
            pltpu.VMEM((1, CELLS), F32),
            pltpu.VMEM((*ends, half, 128), F32),
            pltpu.VMEM((*ends, half, 128), F32),
            pltpu.VMEM((*ends, part, 128), F32),
            pltpu.VMEM((*ends, part, 128), F32),
            pltpu.VMEM((*ends, corner_rows, 128), F32),
            pltpu.VMEM((*ends, half, 128), F32),
            pltpu.VMEM((*ends, half, 128), F32),
            pltpu.VMEM((*ends, part, 128), F32),
            pltpu.VMEM((*ends, part, 128), F32),
            pltpu.VMEM((*ends, 2, corner_rows, 128), F32),
            pltpu.SemaphoreType.DMA((FIELDS + 6,)),
            pltpu.SemaphoreType.DMA((*ends, 6)),
            pltpu.SemaphoreType.DMA((*ends, 6)),
        ],
        compiler_params=pltpu.CompilerParams(
            collective_id=0, has_side_effects=True, vmem_limit_bytes=40 * 1024 * 1024
        ),
        name="diffusion",
    )(
        *(
            pltpu.with_memory_space_constraint(x, pltpu.HBM)
            for x in (
                field, cell_area, dv_edge, dc_edge, cells_on_edge, edges_on_cell, send_cells
            )
        )
    )
    return pl.pallas_call(
        finish,
        out_shape=jax.ShapeDtypeStruct(field.shape, F32),
        in_specs=[vmem] * 6,
        out_specs=hbm,
        scratch_shapes=[
            pltpu.VMEM((FIELDS, LEVELS, CELLS), F32),
            pltpu.SemaphoreType.DMA((FIELDS,)),
        ],
        compiler_params=pltpu.CompilerParams(vmem_limit_bytes=40 * 1024 * 1024),
        name="finish",
    )(*parts, level_coef.reshape(1, -1))


def solution(mesh):
    return jax.shard_map(
        shards,
        mesh=mesh,
        in_specs=(
            P(None, None, "cells"),
            P("cells"),
            P("cells"),
            P("cells"),
            P(None, "cells"),
            P(None, "cells"),
            P(None, "cells"),
            P(),
        ),
        out_specs=P(None, None, "cells"),
        check_vma=False,
    )
```

```python
import functools

import jax
import jax.numpy as jnp
from jax import lax
from jax.experimental import pallas as pl
from jax.experimental.pallas import tpu as pltpu
from jax.sharding import PartitionSpec as P

MESH = pl.DeviceIdType.MESH
F32 = jnp.float32
BF16 = jnp.bfloat16
I32 = jnp.int32
I16 = jnp.int16

BLOCK_ROW = 16
SIDE = 16
SLOT = 64
CELLS = 1024
HALO = 256
FIELDS = 9
LEVELS = 55
PITCH = 56
ROWS = 512
CHUNKS = 2
CHUNK = ROWS // CHUNKS
EDGES = 3232
GROUPS = -(-EDGES // 128)
CORNER_A = CELLS + 192
CORNER_B = CELLS + 224


def dot(a, b):
    return jnp.dot(a, b, preferred_element_type=F32)


def split(x):
    high = x.astype(BF16)
    return high, (x - high.astype(F32)).astype(BF16)


def lanes(shape):
    return lax.broadcasted_iota(I32, shape, 1)


def rows_of(shape):
    return lax.broadcasted_iota(I32, shape, 0)


def kernel(
    field,
    area_in,
    dv_in,
    dc_in,
    ends_in,
    beside_in,
    send_in,
    acc,
    halo_h,
    halo_l,
    rim_h,
    rim_l,
    area,
    dv,
    dc,
    ends,
    beside,
    send,
    xf,
    xh,
    xl,
    select,
    lh,
    ll,
    near,
    coef_h,
    coef_l,
    diag,
    send_up,
    send_down,
    send_right,
    send_left,
    send_corner,
    got_up,
    got_down,
    got_right,
    got_left,
    got_corner,
    load_sem,
    send_sem,
    recv_sem,
):
    count = lax.axis_size("cells")
    me = lax.axis_index("cells")

    def at(offset):
        return lax.rem(me + (offset + count), count)

    offsets = (1, -1, BLOCK_ROW, -BLOCK_ROW, BLOCK_ROW - 1, 1 - BLOCK_ROW)
    barrier = pltpu.get_barrier_semaphore()
    for offset in offsets:
        pl.semaphore_signal(barrier, inc=1, device_id=(at(offset),), device_id_type=MESH)

    def load(i, src, dst):
        copy = pltpu.make_async_copy(src, dst, load_sem.at[i])
        copy.start()
        return copy

    list_load = load(FIELDS, send_in, send)
    table_loads = [
        load(FIELDS + 1 + i, src, dst)
        for i, (src, dst) in enumerate(
            ((beside_in, beside), (ends_in, ends), (dv_in, dv), (dc_in, dc), (area_in, area))
        )
    ]

    loads = [load(f, field.at[f], xf.at[f]) for f in range(FIELDS)]

    list_load.wait()
    lists = send[...]
    wide = (1, 128)
    lane1 = lanes(wide)
    first_cols = jnp.concatenate([lists[2:3], lists[3:4]], axis=1)
    second_cols = jnp.concatenate([lists[0:1], lists[1:2]], axis=1)
    near_cols = jnp.where(lane1 < 16, second_cols, pltpu.roll(second_cols, 80, 1))
    corner_cols = jnp.where(
        lane1 < 96,
        jnp.broadcast_to(lists[4:5, 0:1], wide),
        jnp.broadcast_to(lists[5:6, 0:1], wide),
    )
    second_cols = jnp.where(lane1 < 32, near_cols, jnp.where(lane1 < 64, -1, corner_cols))
    columns = jnp.concatenate([first_cols, second_cols], axis=1)

    def fill_select(i, carry):
        at_row = pl.multiple_of(i * 16, 16)
        ids = rows_of((16, HALO)) + at_row
        select[pl.ds(at_row, 16), :] = jnp.where(ids == columns, 1.0, 0.0).astype(BF16)
        return carry

    lax.fori_loop(0, CELLS // 16, fill_select, 0, unroll=8)

    half = CHUNK // 2
    part = CHUNK // 8
    corner_rows = CHUNK // 32

    def exchange(k, h):
        here = pl.ds(h * CHUNK, CHUNK)
        picked = dot(xh[here, :], select[...]) + dot(xl[here, :], select[...])
        copies = []

        def start(i, src, dst, offset):
            copies.append(
                pltpu.make_async_remote_copy(
                    src_ref=src.at[k, h],
                    dst_ref=dst,
                    send_sem=send_sem.at[k, h, i],
                    recv_sem=recv_sem.at[k, h, i],
                    device_id=(at(offset),),
                    device_id_type=MESH,
                )
            )
            copies[-1].start()

        rest = picked[:, 128:]
        lane32 = lanes((32, 128))
        own = (lane32 >= 64) & ((lane32 & 31) == rows_of((32, 128)))
        folded = [
            jnp.sum(jnp.where(own, rest[32 * g : 32 * g + 32], 0.0), axis=0, keepdims=True)
            for g in range(corner_rows)
        ]
        send_corner[k, h] = jnp.concatenate(folded, axis=0)
        lane = lanes((half, 128))
        top = picked[:half, :128]
        low_half = picked[half:, :128]
        send_up[k, h] = jnp.where(lane < 64, top, pltpu.roll(low_half, 64, 1))
        send_down[k, h] = jnp.where(lane < 64, pltpu.roll(top, 64, 1), low_half)
        if k == 0 and h == 0:
            pl.semaphore_wait(barrier, 6)
        start(4, send_corner, got_corner.at[k, h, 0], offsets[4])
        start(5, send_corner, got_corner.at[k, h, 1], offsets[5])
        start(2, send_up, got_up.at[k, h], offsets[2])
        start(3, send_down, got_down.at[k, h], offsets[3])
        group = lanes((part, 128)) // 16
        right = rest[0:part]
        left = pltpu.roll(rest[0:part], 112, 1)
        for g in range(1, 8):
            piece = rest[part * g : part * g + part]
            right = jnp.where(group == g, pltpu.roll(piece, 16 * g, 1), right)
            left = jnp.where(group == g, piece if g == 1 else pltpu.roll(piece, 16 * g - 16, 1), left)
        send_right[k, h] = right
        send_left[k, h] = left
        start(0, send_right, got_right.at[k, h], offsets[0])
        start(1, send_left, got_left.at[k, h], offsets[1])
        return copies

    def receive(k, h, copies):
        for copy in copies:
            copy.wait_recv()
        lane = lanes((half, 128))
        up = got_up[k, h]
        down = got_down[k, h]
        halo_top = jnp.where(lane < 64, up, pltpu.roll(down, 64, 1))
        halo_low = jnp.where(lane < 64, pltpu.roll(up, 64, 1), down)
        for piece, start in ((halo_top, 0), (halo_low, half)):
            high, low = split(piece)
            halo_h[pl.ds(h * CHUNK + start, half), 0:128] = high
            halo_l[pl.ds(h * CHUNK + start, half), 0:128] = low
        right = got_right[k, h]
        left = got_left[k, h]
        corner_a = got_corner[k, h, 0]
        corner_b = got_corner[k, h, 1]
        shape = (part, 128)
        lane = lanes(shape)
        per_row = 32 // part
        corners = jnp.where(lanes((corner_rows, 128)) < 96, corner_a, corner_b)
        for g in range(8):
            row = g // per_row
            own = (lane & 31) == rows_of(shape) + part * (g % per_row)
            spread = jnp.where(own, jnp.broadcast_to(corners[row : row + 1], shape), 0.0)
            from_left = right if g == 0 else pltpu.roll(right, 128 - 16 * g, 1)
            from_right = left if g == 1 else pltpu.roll(left, (144 - 16 * g) % 128, 1)
            piece = jnp.where(
                lane < 16,
                from_left,
                jnp.where(lane < 32, from_right, jnp.where(lane < 64, 0.0, spread)),
            )
            high, low = split(piece)
            halo_h[pl.ds(h * CHUNK + part * g, part), 128:256] = high
            halo_l[pl.ds(h * CHUNK + part * g, part), 128:256] = low

    for copy in table_loads:
        copy.wait()
    packed = []
    weights = []
    for r in range(GROUPS):
        width = min(128, EDGES - 128 * r)
        where = slice(128 * r, 128 * r + width)
        both = ends[0:1, where] | (ends[1:2, where] << 11)
        ratio = (dv[where] / dc[where]).reshape(1, width)
        if width < 128:
            both = jnp.concatenate([both, jnp.zeros((1, 128 - width), I32)], axis=1)
            ratio = jnp.concatenate([ratio, jnp.zeros((1, 128 - width), F32)], axis=1)
        packed.append(jnp.broadcast_to(both, (8, 128)))
        weights.append(jnp.broadcast_to(ratio, (8, 128)))
    edge_ids = jnp.concatenate([beside[...], jnp.zeros((2, CELLS), I32)], axis=0)
    tile = (8, 128)
    valid = rows_of(tile) < 6
    for t in range(CELLS // 128):
        cols = slice(128 * t, 128 * t + 128)
        ids = edge_ids[:, cols]
        group = ids >> 7
        within = ids & 127
        both = jnp.zeros(tile, I32)
        ratio = jnp.zeros(tile, F32)
        for r in range(GROUPS):
            here = group == r
            both = jnp.where(here, jnp.take_along_axis(packed[r], within, axis=1), both)
            ratio = jnp.where(here, jnp.take_along_axis(weights[r], within, axis=1), ratio)
        end0 = both & 2047
        end1 = both >> 11
        other = jnp.where(end0 == lanes(tile) + 128 * t, end1, end0)
        beyond = other - CELLS
        slot = beyond >> 6
        place = beyond & 63
        start = jnp.where(
            slot == 2,
            CELLS,
            jnp.where(
                slot == 3,
                CELLS + 64,
                jnp.where(
                    slot == 0,
                    CELLS + 128,
                    jnp.where(slot == 1, CELLS + 144, jnp.where(slot == 4, CORNER_A, CORNER_B)),
                ),
            ),
        )
        other = jnp.where(other < CELLS, other, start + place)
        near[:, cols] = jnp.where(valid, other, -1)
        factor = jnp.where(valid, ratio / area[cols].reshape(1, 128), 0.0)
        high, low = (piece.astype(F32) for piece in split(factor))
        coef_h[:, cols] = high
        coef_l[:, cols] = low
        diag[0:1, cols] = jnp.sum(high + low, axis=0, keepdims=True)

    pad = jnp.zeros((PITCH - LEVELS, CELLS), F32)
    acc[FIELDS * PITCH : ROWS, :] = jnp.zeros((ROWS - FIELDS * PITCH, CELLS), F32)
    copies_a = []
    waited = 0
    for h in range(CHUNKS):
        while waited < FIELDS and waited * PITCH < (h + 1) * CHUNK:
            loads[waited].wait()
            acc[pl.ds(waited * PITCH, PITCH), :] = jnp.concatenate([xf[waited], pad], axis=0)
            waited += 1
        here = pl.ds(h * CHUNK, CHUNK)
        high, low = split(acc[here, :])
        xh[here, :] = high
        xl[here, :] = low
        copies_a.append(exchange(0, h))

    block = (16, 128)
    first_ids = rows_of(block).astype(I16)

    def build(t):
        cols = slice(128 * t, 128 * t + 128)
        nears = [jnp.broadcast_to(near[j : j + 1, cols], block).astype(I16) for j in range(6)]
        highs = [jnp.broadcast_to(coef_h[j : j + 1, cols], block).astype(BF16) for j in range(6)]
        lows = [jnp.broadcast_to(coef_l[j : j + 1, cols], block).astype(BF16) for j in range(6)]

        def put(high_ref, low_ref, at_row, ids):
            high = jnp.zeros(block, BF16)
            low = jnp.zeros(block, BF16)
            for j in range(6):
                here = ids == nears[j]
                high = jnp.where(here, highs[j], high)
                low = jnp.where(here, lows[j], low)
            high_ref[at_row : at_row + 16, cols] = high
            low_ref[at_row : at_row + 16, cols] = low

        for at_row in range(0, CELLS, 16):
            put(lh, ll, at_row, first_ids + jnp.full(block, at_row, I16))
        for at_row in range(0, HALO, 16):
            ids = first_ids + jnp.full(block, CELLS + at_row, I16)
            if CELLS + at_row >= CORNER_A:
                corner = CORNER_A if CELLS + at_row < CORNER_B else CORNER_B
                ids = jnp.full(block, corner, I16)
            put(rim_h, rim_l, at_row, ids)

    tiles = [slice(256 * n, 256 * n + 256) for n in range(CELLS // 256)]

    def own_part(building=False):
        for n, cols in enumerate(tiles):
            if building and n + 1 < len(tiles):
                build(2 * n + 2)
                build(2 * n + 3)
            a = dot(xh[...], lh[:, cols])
            a += dot(xh[...], ll[:, cols])
            a += dot(xl[...], lh[:, cols])
            acc[:, cols] = a - diag[0:1, cols] * acc[:, cols]

    def halo_part(h, then=None):
        here = pl.ds(h * CHUNK, CHUNK)
        for cols in tiles:
            a = dot(halo_h[here, :], rim_h[:, cols])
            a += dot(halo_h[here, :], rim_l[:, cols])
            a += dot(halo_l[here, :], rim_h[:, cols])
            value = acc[here, cols] + a
            acc[here, cols] = value
            if then is not None:
                then(here, cols, value)

    def keep(here, cols, value):
        high, low = split(value)
        xh[here, cols] = high
        xl[here, cols] = low

    build(0)
    build(1)
    own_part(building=True)
    copies_b = []
    for h in range(CHUNKS):
        receive(0, h, copies_a[h])
        halo_part(h, keep)
        copies_b.append(exchange(1, h))
    own_part()
    for h in range(CHUNKS):
        receive(1, h, copies_b[h])
        if h < CHUNKS - 1:
            halo_part(h)
    for h in range(CHUNKS):
        for copy in copies_a[h] + copies_b[h]:
            copy.wait_send()


def finish(acc, halo_h, halo_l, rim_h, rim_l, level, out, result, sem):
    spread = jnp.broadcast_to(level[...], (LEVELS, LEVELS))
    on_diagonal = lanes((LEVELS, LEVELS)) == rows_of((LEVELS, LEVELS))
    scale = -jnp.sum(jnp.where(on_diagonal, spread, 0.0), axis=1, keepdims=True)
    last = (CHUNKS - 1) * CHUNK
    copies = []

    def put(f):
        copies.append(pltpu.make_async_copy(result.at[f], out.at[f], sem.at[f]))
        copies[-1].start()

    for f in range(FIELDS):
        start = f * PITCH
        ready = min(LEVELS, max(0, last - start))
        if ready:
            result[f, 0:ready, :] = acc[start : start + ready, :] * scale[0:ready]
        if ready == LEVELS:
            put(f)
    early = len(copies)
    tail = pl.ds(last, CHUNK)
    for n in range(CELLS // 256):
        cols = slice(256 * n, 256 * n + 256)
        a = dot(halo_h[tail, :], rim_h[:, cols])
        a += dot(halo_h[tail, :], rim_l[:, cols])
        a += dot(halo_l[tail, :], rim_h[:, cols])
        value = acc[tail, cols] + a
        for f in range(FIELDS):
            start = f * PITCH
            ready = min(LEVELS, max(0, last - start))
            if ready < LEVELS:
                result[f, ready:LEVELS, cols] = (
                    value[start + ready - last : start + LEVELS - last] * scale[ready:LEVELS]
                )
        rest = pl.ds(early, FIELDS - early)
        copies.append(
            pltpu.make_async_copy(
                result.at[rest, :, cols], out.at[rest, :, cols], sem.at[early + n]
            )
        )
        copies[-1].start()
    for copy in copies:
        copy.wait()


def shards(
    field, cell_area, dv_edge, dc_edge, cells_on_edge, edges_on_cell, send_cells, level_coef
):
    vmem = pl.BlockSpec(memory_space=pltpu.VMEM)
    hbm = pl.BlockSpec(memory_space=pltpu.HBM)
    half = CHUNK // 2
    part = CHUNK // 8
    corner_rows = CHUNK // 32
    ends = (2, CHUNKS)
    parts = pl.pallas_call(
        kernel,
        out_shape=[
            jax.ShapeDtypeStruct((ROWS, CELLS), F32),
            jax.ShapeDtypeStruct((ROWS, HALO), BF16),
            jax.ShapeDtypeStruct((ROWS, HALO), BF16),
            jax.ShapeDtypeStruct((HALO, CELLS), BF16),
            jax.ShapeDtypeStruct((HALO, CELLS), BF16),
        ],
        in_specs=[hbm] * 7,
        out_specs=[vmem] * 5,
        scratch_shapes=[
            pltpu.VMEM((CELLS,), F32),
            pltpu.VMEM((EDGES,), F32),
            pltpu.VMEM((EDGES,), F32),
            pltpu.VMEM((2, EDGES), I32),
            pltpu.VMEM((6, CELLS), I32),
            pltpu.VMEM((6, SLOT), I32),
            pltpu.VMEM((FIELDS, LEVELS, CELLS), F32),
            pltpu.VMEM((ROWS, CELLS), BF16),
            pltpu.VMEM((ROWS, CELLS), BF16),
            pltpu.VMEM((CELLS, HALO), BF16),
            pltpu.VMEM((CELLS, CELLS), BF16),
            pltpu.VMEM((CELLS, CELLS), BF16),
            pltpu.VMEM((8, CELLS), I32),
            pltpu.VMEM((8, CELLS), F32),
            pltpu.VMEM((8, CELLS), F32),
            pltpu.VMEM((1, CELLS), F32),
            pltpu.VMEM((*ends, half, 128), F32),
            pltpu.VMEM((*ends, half, 128), F32),
            pltpu.VMEM((*ends, part, 128), F32),
            pltpu.VMEM((*ends, part, 128), F32),
            pltpu.VMEM((*ends, corner_rows, 128), F32),
            pltpu.VMEM((*ends, half, 128), F32),
            pltpu.VMEM((*ends, half, 128), F32),
            pltpu.VMEM((*ends, part, 128), F32),
            pltpu.VMEM((*ends, part, 128), F32),
            pltpu.VMEM((*ends, 2, corner_rows, 128), F32),
            pltpu.SemaphoreType.DMA((FIELDS + 6,)),
            pltpu.SemaphoreType.DMA((*ends, 6)),
            pltpu.SemaphoreType.DMA((*ends, 6)),
        ],
        compiler_params=pltpu.CompilerParams(
            collective_id=0, has_side_effects=True, vmem_limit_bytes=40 * 1024 * 1024
        ),
        name="diffusion",
    )(
        *(
            pltpu.with_memory_space_constraint(x, pltpu.HBM)
            for x in (
                field, cell_area, dv_edge, dc_edge, cells_on_edge, edges_on_cell, send_cells
            )
        )
    )
    return pl.pallas_call(
        finish,
        out_shape=jax.ShapeDtypeStruct(field.shape, F32),
        in_specs=[vmem] * 6,
        out_specs=hbm,
        scratch_shapes=[
            pltpu.VMEM((FIELDS, LEVELS, CELLS), F32),
            pltpu.SemaphoreType.DMA((FIELDS,)),
        ],
        compiler_params=pltpu.CompilerParams(vmem_limit_bytes=40 * 1024 * 1024),
        name="finish",
    )(*parts, level_coef.reshape(1, -1))


def solution(mesh):
    return jax.shard_map(
        shards,
        mesh=mesh,
        in_specs=(
            P(None, None, "cells"),
            P("cells"),
            P("cells"),
            P("cells"),
            P(None, "cells"),
            P(None, "cells"),
            P(None, "cells"),
            P(),
        ),
        out_specs=P(None, None, "cells"),
        check_vma=False,
    )
```
